32 devices in a mesh: band: 2 (over x), domain: 16 (over z, y, core).
Axes of the slice: x: 2, y: 2, z: 4, core: 2. Of those that a mesh axis runs over, the one named last changes fastest.
Arguments:
- dens_part: float32 [2, 171, 36864], P('band', None, 'domain'), may hold values from -3 to 3
- counts: int32 [16], P('domain'), may hold values from 1 to 2304, 12288 in all
- gaunt: float32 [171, 525], replicated, may hold values from -0.4375 to 0.4375
- pair_waves: float32 [21, 400], replicated, may hold values from -1.25 to 1.25
- y_table: float32 [25, 50], replicated, may hold values from -1.25 to 1.25
- core: float32 [400], replicated, may hold values from 1 to 4
- radial_weights: float32 [400], replicated, may hold values from 0.0001 to 0.001
Outputs:
- dh_packed: float32 [171, 36864], P(None, 'domain')
- atom_energy: float32 [36864], P('domain')
The draws below stay inside these ranges and needn't reach their ends.
Inputs may be any that keep to these rules, and one draw needn't show every extreme that they name: `counts`: atoms owned by each domain; they sum to 12288, and some domain owns exactly 2304.
All inputs are finite; a program needn't handle non-finite values. No bound on the sum of `counts` on one device may be relied on, other than what follows from the above.
Results may differ from the reference program's by a relative error of at most 0.0003.
Values sent between devices are 32-bit elements; how exact they have to be, the bound alone decides.
A program may use at most 128 MiB of HBM per device.

```python
import math
import jax
import jax.numpy as jnp
import numpy as np
from jax import lax

NP = 171
NQ = 21
LM = 25
NDIR = 50
G = 400
ATOM_DEV = 768
SLOTS = 2304
N_BAND = 2
N_DOMAIN = 16


def block_levels(own_key, shape, shards, smallest, high):
    level = 1.0
    for position, parts in shards:
        steps = jax.random.uniform(jax.random.fold_in(jax.random.fold_in(own_key, 6), position), (parts,), jnp.float32, smallest / len(shards), high / len(shards))
        level = level * jnp.repeat(jnp.exp(steps), shape[position] // parts).reshape((-1,) + (1,) * (len(shape) - 1 - position))
    return level


def profile(amount, total, bound, skew):
    portions = [(1 << 20) // math.isqrt(grade ** skew) + 1 for grade in range(2, amount + 1)]
    rest, given = total - bound - (amount - 1), [1] * (amount - 1)
    while rest > 0:
        movable = [i for i in range(amount - 1) if given[i] < bound]
        pool, left = sum([portions[i] for i in movable]), rest
        for i in movable:
            more = min(bound - given[i], max(1, left * portions[i] // pool), rest)
            given[i] = given[i] + more
            rest = rest - more
    return np.array([bound] + given)


def ragged_sizes(own_key, count, total, limit, lean):
    if count == 2:
        one = jax.random.randint(own_key, (), max(1, total - limit), min(limit, total - 1) + 1)
        return jnp.stack([one, total - one])
    tallies = jnp.asarray(profile(count, total, limit, lean), jnp.int32)
    couples = (count - 1) // 2
    source_of, taker = tallies[1:1 + 2 * couples:2], tallies[2:2 + 2 * couples:2]
    room = jnp.minimum(source_of - 1, limit - taker)
    passed = jax.random.randint(jax.random.fold_in(own_key, 1), (couples,), 0, 1 << 20) % (room + 1)
    tallies = tallies.at[1:1 + 2 * couples:2].set(source_of - passed).at[2:2 + 2 * couples:2].set(taker + passed)
    return tallies[jax.random.permutation(jax.random.fold_in(own_key, 2), count)]


def bell_draw(rng, shape, scale, limit, split=(), held_as=jnp.bfloat16):
    array = scale * jax.random.normal(rng, shape, jnp.float32)
    if split:
        array = array * block_levels(rng, shape, split, -0.22, 0.18)
    return jnp.clip(array, -limit, limit).astype(held_as)


def setup_inputs(seed: int = 0) -> dict:
    streams_of = jax.random.split(jax.random.key(seed), 8)
    dens_part = bell_draw(streams_of[0], (N_BAND, NP, N_DOMAIN * SLOTS), 0.35, 3.0, ((0, 2), (2, 16)), jnp.float32)
    counts = ragged_sizes(streams_of[1], N_DOMAIN, ATOM_DEV * N_DOMAIN, SLOTS, 2).astype(jnp.int32)
    gaunt = bell_draw(streams_of[2], (NP, LM * NQ), NP ** -0.5, 0.4375, (), jnp.float32)
    pair_waves = bell_draw(streams_of[3], (NQ, G), NQ ** -0.5, 1.25, (), jnp.float32)
    y_table = bell_draw(streams_of[4], (LM, NDIR), LM ** -0.5, 1.25, (), jnp.float32)
    core = jnp.clip(jnp.exp(jax.random.uniform(streams_of[5], (G,), jnp.float32, math.log(1.0), math.log(4.0))), 1.0, 4.0)
    radial_weights = jnp.clip(jnp.exp(jax.random.uniform(streams_of[6], (G,), jnp.float32, math.log(0.0001), math.log(0.001))), 0.0001, 0.001)
    return {"dens_part": dens_part, "counts": counts, "gaunt": gaunt, "pair_waves": pair_waves, "y_table": y_table, "core": core, "radial_weights": radial_weights}


highest = lax.Precision.HIGHEST

def local_energy(density_rows, gaunt, pair_waves, y_table, core, radial_weights):
    atom_count = density_rows.shape[0]
    harmonics = y_table.shape[0]
    pair_count = pair_waves.shape[0]
    directions = y_table.shape[1]
    coefficients = jnp.dot(density_rows, gaunt, precision=highest, preferred_element_type=jnp.float32)
    coefficients = coefficients.reshape(atom_count * harmonics, pair_count)
    radial = jnp.dot(coefficients, pair_waves, precision=highest, preferred_element_type=jnp.float32)
    radial = radial.reshape(atom_count, harmonics, pair_waves.shape[1])
    points = jnp.einsum('ln,alg->ang', y_table, radial, precision=highest) + core[None, None, :]
    smooth = jnp.sqrt(points * points + 0.25)
    cube_root = jnp.cbrt(smooth)
    wigner_radius = 0.6203504908994 / cube_root
    denominator = 7.8 + wigner_radius
    energy_density = -0.7385587663820224 * smooth * cube_root - 0.44 * smooth / denominator
    slope = -0.9847450218426965 * cube_root - 0.44 * (1.0 / denominator + wigner_radius / (3.0 * denominator * denominator))
    point_weight = 4.0 * jnp.pi / directions * radial_weights
    energy = lax.optimization_barrier(jnp.sum(energy_density * point_weight[None, None, :], axis=(1, 2)))
    potential = point_weight[None, None, :] * slope * points / smooth
    back_radial = jnp.einsum('ln,ang->alg', y_table, potential, precision=highest)
    back_coef = jnp.dot(back_radial.reshape(atom_count * harmonics, pair_waves.shape[1]), pair_waves.T, precision=highest, preferred_element_type=jnp.float32)
    back_coef = back_coef.reshape(atom_count, harmonics * pair_count)
    hamiltonian = jnp.dot(back_coef, gaunt.T, precision=highest, preferred_element_type=jnp.float32)
    return (hamiltonian, energy)

def reference(dens_part, counts, gaunt, pair_waves, y_table, core, radial_weights):
    density = lax.optimization_barrier(jnp.sum(dens_part, axis=0)).T.reshape(N_DOMAIN, SLOTS, NP)
    slot_ids = jnp.arange(SLOTS).astype(jnp.int32)

    def per_domain(packed):
        block, owned = packed
        is_alive = slot_ids < owned
        block = jnp.where(is_alive[:, None], block, jnp.zeros_like(block))
        hamiltonian, energy = local_energy(block, gaunt, pair_waves, y_table, core, radial_weights)
        hamiltonian = jnp.where(is_alive[:, None], hamiltonian, jnp.zeros_like(hamiltonian))
        energy = jnp.where(is_alive, energy, jnp.zeros_like(energy))
        return (hamiltonian, energy)
    hamiltonian, energy = lax.map(per_domain, (density, counts.astype(jnp.int32)))
    return (hamiltonian.reshape(N_DOMAIN * SLOTS, NP).T, energy.reshape(N_DOMAIN * SLOTS))
```

```python
import math

import jax
import jax.numpy as jnp
from jax import lax
from jax.experimental import pallas as pl
from jax.experimental.pallas import tpu as pltpu
from jax.sharding import PartitionSpec as P

highest = lax.Precision.HIGHEST
f32 = jnp.float32
bf16 = jnp.bfloat16

LANES = 128
WIDE = 256

C_RS = 0.6203504908994
EX_A = 0.7385587663820224
EX_D = 0.9847450218426965

def round_up(value, step):
    return -(-value // step) * step

def split(x):
    hi = lax.reduce_precision(x, 8, 7)
    return hi.astype(bf16), (x - hi).astype(bf16)

def general_kernel(
    dens_ref, gy_ref, gyb_ref, pw_ref, pwb_ref, core_ref, weight_ref,
    ham_ref, energy_ref, pts_ref, hi_ref, lo_ref, eacc_ref, back_ref, *, pairs, step
):
    atoms = dens_ref.shape[1]
    rows = pw_ref.shape[1]
    grid_points = pw_ref.shape[0]
    couples = gy_ref.shape[0]
    chunks = 2 * atoms // WIDE
    eacc_ref[...] = jnp.zeros_like(eacc_ref)

    def mixed(x):
        ids = lax.broadcasted_iota(jnp.int32, x.shape, 0)
        hi = x.astype(bf16).astype(f32)
        low = (ids >= pairs) & (ids < 2 * pairs)
        return jnp.where(low, x - hi, hi).astype(bf16)

    def body(m, carry):
        both = jnp.dot(gy_ref[m], dens_ref[...], preferred_element_type=f32)
        lhs = mixed(jnp.concatenate([both[:rows], both[rows:]], axis=1))
        back = []
        for j in range(chunks):
            cols = lhs[:, j * WIDE:(j + 1) * WIDE]
            pts_ref[j] = jnp.dot(pw_ref[...], cols, preferred_element_type=f32)
            for g in range(0, grid_points, step):
                part = pl.ds(g, step)
                p = pts_ref[j, part, :] + core_ref[part, :]
                u = p * p + 0.25
                v = jnp.exp2(jnp.log(u) * (-1.0 / (6.0 * math.log(2.0))))
                r = v / (7.8 + C_RS * v)
                v2 = v * v
                br = 0.44 * r
                eacc_ref[j, part, :] += (u * v2) * (EX_A + br)
                pot = (p * v2) * (EX_D + (0.44 + (0.44 * C_RS / 3.0) * r) * r)
                hi = pot.astype(bf16)
                hi_ref[j, part, :] = hi
                lo_ref[j, part, :] = (pot - hi.astype(f32)).astype(bf16)
            first = jnp.dot(pwb_ref[...], hi_ref[j], preferred_element_type=f32)
            second = jnp.dot(pwb_ref[:rows, :], lo_ref[j], preferred_element_type=f32)
            back.append(first[:rows] + first[rows:] + second)
        back = mixed(jnp.concatenate(back, axis=1))
        start = pl.multiple_of(m * 2 * rows, 2 * rows)
        back_ref[pl.ds(start, rows), :] = back[:, :atoms]
        back_ref[pl.ds(start + rows, rows), :] = back[:, atoms:]
        return carry

    lax.fori_loop(0, couples, body, 0)
    ham_ref[...] = jnp.dot(gyb_ref[...], back_ref[...], preferred_element_type=f32)
    sums = [
        jnp.sum(eacc_ref[j] * weight_ref[...], axis=0, keepdims=True) for j in range(chunks)
    ]
    sums = jnp.concatenate(sums, axis=1)
    energy_ref[...] = jnp.broadcast_to(
        -(sums[:, :atoms] + sums[:, atoms:]), energy_ref.shape
    )

def general_tables(gaunt, pair_waves, y_table, core, radial_weights):
    entries = gaunt.shape[0]
    harmonics, directions = y_table.shape
    pairs, grid_points = pair_waves.shape
    rows = round_up(3 * pairs, 16)
    extra = rows - 3 * pairs
    assert directions % 2 == 0
    fused = jnp.einsum(
        "plq,ln->nqp", gaunt.reshape(entries, harmonics, pairs), y_table, precision=highest
    )

    hi, lo = split(fused)
    wide = lambda a, b, c: jnp.pad(
        jnp.concatenate([a, b, c], axis=1), ((0, 0), (0, extra), (0, 0))
    )
    hi3 = wide(hi, hi, hi)
    lo3 = wide(lo, lo, lo)
    gy = jnp.concatenate([hi3, hi3, lo3], axis=2).reshape(directions // 2, 2 * rows, 3 * entries)
    gyb = wide(hi, hi, lo).reshape(directions * rows, entries).T
    pw_hi, pw_lo = split(pair_waves)
    pw = jnp.pad(jnp.concatenate([pw_hi, pw_hi, pw_lo], axis=0), ((0, extra), (0, 0))).T
    point_weight = 4.0 * jnp.pi / directions * radial_weights
    b_hi, b_lo = split(-point_weight[None, :] * pair_waves)
    triple = lambda x: jnp.pad(jnp.concatenate([x, x, x], axis=0), ((0, extra), (0, 0)))
    pwb = jnp.concatenate([triple(b_hi), triple(b_lo)], axis=0)
    core_wide = jnp.broadcast_to(core[:, None], (grid_points, WIDE))
    weight_wide = jnp.broadcast_to(point_weight[:, None], (grid_points, WIDE))
    return gy, gyb, pw, pwb, core_wide, weight_wide

def general_energy(columns, tables, pairs):
    entries, atoms = columns.shape
    gy, gyb, pw, pwb, core_wide, weight_wide = tables
    grid_points, rows = pw.shape
    hi, lo = split(columns)
    dens = jnp.concatenate([hi, lo, hi], axis=0)
    chunks = 2 * atoms // WIDE
    step = 80 if grid_points % 80 == 0 else grid_points

    ham, energy = pl.pallas_call(
        lambda *refs: general_kernel(*refs, pairs=pairs, step=step),
        out_shape=(
            jax.ShapeDtypeStruct((entries, atoms), f32),
            jax.ShapeDtypeStruct((8, atoms), f32),
        ),
        scratch_shapes=[
            pltpu.VMEM((chunks, grid_points, WIDE), f32),
            pltpu.VMEM((chunks, grid_points, WIDE), bf16),
            pltpu.VMEM((chunks, grid_points, WIDE), bf16),
            pltpu.VMEM((chunks, grid_points, WIDE), f32),
            pltpu.VMEM((gyb.shape[1], atoms), bf16),
        ],
        compiler_params=pltpu.CompilerParams(vmem_limit_bytes=48 * 1024 * 1024),
        name="atoms",
    )(dens, gy, gyb, pw, pwb, core_wide, weight_wide)
    return ham, energy[:1]

def general(dens_part, counts, gaunt, pair_waves, y_table, core, radial_weights):
    band_count = lax.axis_size("band")
    domain_count = lax.axis_size("domain")
    workers = band_count * domain_count
    axes = ("domain", "band")
    me = lax.axis_index("domain") * band_count + lax.axis_index("band")
    entries = dens_part.shape[1]
    slot_total = dens_part.shape[2]
    share = slot_total // band_count
    capacity = -(-share // workers)
    worker_rows = -(-(slot_total // 3) // band_count)
    atoms = round_up(worker_rows, LANES)
    tables = general_tables(gaunt, pair_waves, y_table, core, radial_weights)

    own_cols = lax.psum_scatter(dens_part[0], "band", scatter_dimension=1, tiled=True)
    every_count = lax.all_gather(counts, "domain", axis=0, tiled=True)
    band_ids = jnp.arange(band_count, dtype=jnp.int32)
    live = jnp.clip(every_count[:, None] - band_ids[None, :] * share, 0, share).reshape(-1)
    ids = jnp.arange(workers, dtype=jnp.int32)
    starts = jnp.sum(jnp.where(ids[None, :] < ids[:, None], live[None, :], 0), axis=1)
    ends = starts + live
    own_start = jnp.sum(jnp.where(ids == me, starts, 0))
    own_live = jnp.sum(jnp.where(ids == me, live, 0))
    is_alive = jnp.arange(share, dtype=jnp.int32) < own_live

    own_cols = jnp.where(is_alive[None, :], own_cols, 0.0)
    own_cols = jnp.pad(own_cols, ((0, 0), (0, capacity * workers - share)))
    blocks = own_cols.T.reshape(capacity, workers, entries).transpose(1, 0, 2)
    outgoing = jnp.roll(blocks, own_start % workers, axis=0)
    incoming = lax.all_to_all(outgoing, axes, split_axis=0, concat_axis=0, tiled=True)

    atom_ids = jnp.arange(atoms, dtype=jnp.int32) * workers + me
    source = jnp.sum((ends[None, :] <= atom_ids[:, None]).astype(jnp.int32), axis=1)
    source = jnp.minimum(source, workers - 1)
    source_start = jnp.sum(jnp.where(source[:, None] == ids[None, :], starts[None, :], 0), axis=1)
    position = jnp.clip((atom_ids - source_start) // workers, 0, capacity - 1)
    compact = jnp.take(
        incoming.reshape(workers * capacity, entries), source * capacity + position, axis=0,
        mode="clip",
    )
    ham, energy = general_energy(compact.T, tables, pair_waves.shape[0])
    result = jnp.concatenate([ham, energy], axis=0).T
    row = (me - starts) % workers
    first = (starts + row - me) // workers
    target = first[:, None] + jnp.arange(capacity, dtype=jnp.int32)[None, :]
    back = jnp.take(result, jnp.clip(target, 0, atoms - 1).reshape(-1), axis=0, mode="clip")
    returned = lax.all_to_all(
        back.reshape(workers, capacity, entries + 1), axes, split_axis=0, concat_axis=0, tiled=True
    )
    returned = jnp.roll(returned, -(own_start % workers), axis=0)
    piece = returned.transpose(1, 0, 2).reshape(capacity * workers, entries + 1)[:share]
    piece = jnp.where(is_alive[:, None], piece, 0.0)
    band = lax.axis_index("band")
    whole = jnp.zeros((slot_total, entries + 1), f32)
    ring = [(i, (i + 1) % band_count) for i in range(band_count)]
    for hop in range(band_count):
        owner = (band - hop) % band_count
        whole = lax.dynamic_update_slice(whole, piece, (owner * share, 0))
        if hop + 1 < band_count:
            piece = lax.ppermute(piece, "band", ring)
    whole = whole.T
    return whole[:entries], whole[entries]

MESH = pl.DeviceIdType.MESH
SUBLANES = 8
TAIL = 64

def chunk_plan(slots, width):
    windows = slots // width
    return [range(k, min(k + 2, windows)) for k in range(0, windows, 2)]

def dot_last(a, b):
    return lax.dot_general(a, b, (((1,), (1,)), ((), ())), preferred_element_type=f32)

def two(x):
    hi = x.astype(bf16)
    return hi, (x - hi.astype(f32)).astype(bf16)

def greet(domains, domain, band):
    barrier = pltpu.get_barrier_semaphore()

    def hello(off, carry):
        peer = lax.rem(domain + off, domains)
        pl.semaphore_signal(barrier, inc=1, device_id=(band, peer), device_id_type=MESH)
        return carry

    lax.fori_loop(1, domains, hello, 0)
    pl.semaphore_signal(barrier, inc=1, device_id=(1 - band, domain), device_id_type=MESH)
    pl.semaphore_wait(barrier, domains)

def scatter_kernel(
    dens_ref, cnt_ref, recv_ref, all_ref, perm_ref, stage, send, cross,
    cnt_out, cnt_in, x_out, x_in, a_out, a_in, *, domains
):
    band, domain = lax.axis_index("band"), lax.axis_index("domain")
    entries, slots = dens_ref.shape
    workers = 2 * domains
    half = SUBLANES * domains
    width = 2 * half
    chunks = chunk_plan(slots, width)
    extra = entries - LANES
    greet(domains, domain, band)

    def count_copy(off):
        peer = lax.rem(domain + off, domains)
        return pltpu.make_async_remote_copy(
            src_ref=cnt_ref, dst_ref=all_ref.at[domain], send_sem=cnt_out.at[off],
            recv_sem=cnt_in.at[off], device_id=(band, peer), device_id_type=MESH,
        )

    def loop(first, function):
        def step(off, carry):
            function(off)
            return carry
        lax.fori_loop(first, domains, step, 0)

    loop(1, lambda off: count_copy(off).start())
    all_ref[domain] = cnt_ref[...]
    stage[...] = jnp.zeros_like(stage)
    loop(1, lambda off: count_copy(off).wait_recv())
    start = jnp.zeros((SUBLANES, LANES), jnp.int32)
    for d in range(domains):
        start = start + jnp.where(d < domain, all_ref[d], 0)
    start = start[:1, :1]
    row = lax.broadcasted_iota(jnp.int32, (width, width), 0)
    slot = lax.broadcasted_iota(jnp.int32, (width, width), 1)
    own = row < half
    row = jnp.where(own, row, row - half)
    worker = 2 * (row // SUBLANES) + jnp.where(own, band, 1 - band)
    source = ((worker - start) & (workers - 1)) + workers * (row % SUBLANES)
    perm = jnp.where(slot == source, 1.0, 0.0).astype(bf16)
    perm_ref[...] = perm

    def cross_copy(c):
        lanes = (len(chunks[c]) + 1) * LANES
        return pltpu.make_async_remote_copy(
            src_ref=send.at[c, pl.ds(half, half), pl.ds(0, lanes)],
            dst_ref=cross.at[c, :, pl.ds(0, lanes)], send_sem=x_out.at[c],
            recv_sem=x_in.at[c], device_id=(1 - band, domain), device_id_type=MESH,
        )

    def deal_copy(c, off):
        lanes = (len(chunks[c]) + 1) * LANES
        peer = lax.rem(domain + off, domains)
        rows = pl.ds(pl.multiple_of(peer * SUBLANES, SUBLANES), SUBLANES)
        there = pl.ds(pl.multiple_of(domain * SUBLANES, SUBLANES), SUBLANES)
        return pltpu.make_async_remote_copy(
            src_ref=send.at[c, rows, pl.ds(0, lanes)],
            dst_ref=recv_ref.at[c, there, pl.ds(0, lanes)], send_sem=a_out.at[c, off],
            recv_sem=a_in.at[c, off], device_id=(band, peer), device_id_type=MESH,
        )

    for c, windows in enumerate(chunks):
        base = len(windows) * LANES
        for i, k in enumerate(windows):
            part = pl.ds(k * width, width)
            stage[i * LANES:(i + 1) * LANES, :] = dens_ref[:LANES, part]
            stage[base + i * TAIL:base + i * TAIL + extra, :] = dens_ref[LANES:, part]
        if len(windows) == 1:
            stage[base + TAIL:base + 2 * TAIL, :] = jnp.zeros((TAIL, width), f32)
            stage[base + extra:base + TAIL, :] = jnp.zeros((TAIL - extra, width), f32)
        hi, lo = two(stage[:base + LANES, :])
        send[c, :, :base + LANES] = dot_last(perm, hi) + dot_last(perm, lo)
        cross_copy(c).start()
    mine = pl.ds(pl.multiple_of(domain * SUBLANES, SUBLANES), SUBLANES)
    for c, windows in enumerate(chunks):
        lanes = (len(windows) + 1) * LANES
        cross_copy(c).wait_recv()
        send[c, :half, :lanes] += cross[c, :, :lanes]
        loop(1, lambda off: deal_copy(c, off).start())
        recv_ref[c, mine, :lanes] = send[c, mine, :lanes]
        if lanes < recv_ref.shape[2]:
            recv_ref[c, :, lanes:] = jnp.zeros((half, recv_ref.shape[2] - lanes), f32)
    for c in range(len(chunks)):
        loop(1, lambda off: deal_copy(c, off).wait_recv())
    for c in range(len(chunks)):
        loop(1, lambda off: deal_copy(c, off).wait_send())
        cross_copy(c).wait_send()
    loop(1, lambda off: count_copy(off).wait_send())

def gather_kernel(
    res_ref, perm_ref, ham_ref, energy_ref, got, cross, x_out, x_in, a_out, a_in, *, domains
):
    band, domain = lax.axis_index("band"), lax.axis_index("domain")
    entries, slots = ham_ref.shape
    half = SUBLANES * domains
    width = 2 * half
    chunks = chunk_plan(slots, width)
    extra = entries - LANES
    greet(domains, domain, band)

    def loop(first, function):
        def step(off, carry):
            function(off)
            return carry
        lax.fori_loop(first, domains, step, 0)

    def back_copy(c, off):
        lanes = (len(chunks[c]) + 1) * LANES
        peer = lax.rem(domain + off, domains)
        rows = pl.ds(pl.multiple_of(peer * SUBLANES, SUBLANES), SUBLANES)
        there = pl.ds(pl.multiple_of(domain * SUBLANES, SUBLANES), SUBLANES)
        return pltpu.make_async_remote_copy(
            src_ref=res_ref.at[c, rows, pl.ds(0, lanes)],
            dst_ref=got.at[c, there, pl.ds(0, lanes)], send_sem=a_out.at[c, off],
            recv_sem=a_in.at[c, off], device_id=(band, peer), device_id_type=MESH,
        )

    def cross_copy(c):
        lanes = (len(chunks[c]) + 1) * LANES
        return pltpu.make_async_remote_copy(
            src_ref=got.at[c, :, pl.ds(0, lanes)],
            dst_ref=cross.at[c, :, pl.ds(0, lanes)], send_sem=x_out.at[c],
            recv_sem=x_in.at[c], device_id=(1 - band, domain), device_id_type=MESH,
        )

    for c in range(len(chunks)):
        loop(1, lambda off: back_copy(c, off).start())
    mine = pl.ds(pl.multiple_of(domain * SUBLANES, SUBLANES), SUBLANES)
    for c in range(len(chunks)):
        got[c, mine, :] = res_ref[c, mine, :]
    perm = perm_ref[...]

    def finish(c):
        cross_copy(c).wait_recv()
        windows = chunks[c]
        base = len(windows) * LANES

        def spread(lanes):
            rows = jnp.concatenate([got[c, :, lanes], cross[c, :, lanes]], axis=0).T
            hi, lo = two(rows)
            return jnp.dot(hi, perm, preferred_element_type=f32) + jnp.dot(
                lo, perm, preferred_element_type=f32
            )

        tails = spread(slice(base, base + LANES))
        for i, k in enumerate(windows):
            part = pl.ds(k * width, width)
            ham_ref[:LANES, part] = spread(slice(i * LANES, (i + 1) * LANES))
            ham_ref[LANES:, part] = tails[i * TAIL:i * TAIL + extra]
            energy_ref[:, part] = tails[i * TAIL + extra:i * TAIL + extra + 1]

    for c in range(len(chunks)):
        loop(1, lambda off: back_copy(c, off).wait_recv())
        cross_copy(c).start()
        if c:
            finish(c - 1)
    finish(len(chunks) - 1)
    for c in range(len(chunks)):
        loop(1, lambda off: back_copy(c, off).wait_send())
        cross_copy(c).wait_send()

def atom_kernel(
    me_ref, recv_ref, all_ref, gy_ref, gyb_ref, pw_ref, pwb_ref, core_ref, weight_ref,
    res_ref, sel_ref, stack_ref, dens_ref, pts_ref, hi_ref, lo_ref, eacc_ref, back_ref,
    *, pairs, step, entries, domains, slots
):
    atoms = dens_ref.shape[1]
    rows = pw_ref.shape[1]
    grid_points = pw_ref.shape[0]
    couples = gy_ref.shape[0]
    packed = LANES + TAIL
    workers = 2 * domains
    half = SUBLANES * domains
    width = 2 * half
    chunks = chunk_plan(slots, width)
    columns = 2 * atoms // WIDE
    eacc_ref[...] = jnp.zeros_like(eacc_ref)

    row = lax.broadcasted_iota(jnp.int32, (half, LANES), 0)
    start = jnp.zeros((half, LANES), jnp.int32)
    count = jnp.zeros((half, LANES), jnp.int32)
    for d in range(domains):
        value = all_ref[d][:1, :]
        start = start + jnp.where(row >= (d + 1) * SUBLANES, value, 0)
        count = jnp.where(row // SUBLANES == d, value, count)
    first = ((me_ref[0] - start) & (workers - 1)) + workers * (row % SUBLANES)
    lane = lax.broadcasted_iota(jnp.int32, (half, atoms), 1)
    for c, windows in enumerate(chunks):
        base = len(windows) * LANES
        tails = recv_ref[c, :, base:base + LANES].T
        for i, k in enumerate(windows):
            slot = first + k * width
            place = jnp.where(slot < count, (start + slot) // workers, -1)
            place = jnp.concatenate([place] * (atoms // LANES), axis=1)
            spot = slice(k * half, (k + 1) * half)
            sel_ref[spot, :] = jnp.where(place == lane, 1.0, 0.0).astype(bf16)
            stack_ref[:LANES, spot] = recv_ref[c, :, i * LANES:(i + 1) * LANES].T
            stack_ref[LANES:, spot] = tails[i * TAIL:(i + 1) * TAIL]
    hi, lo = two(stack_ref[...])
    hi = jnp.dot(hi, sel_ref[...], preferred_element_type=f32).astype(bf16)
    lo = jnp.dot(lo, sel_ref[...], preferred_element_type=f32).astype(bf16)
    dens_ref[:packed, :] = hi
    dens_ref[packed:2 * packed, :] = lo
    dens_ref[2 * packed:, :] = hi

    def mixed(x):
        ids = lax.broadcasted_iota(jnp.int32, x.shape, 0)
        hi = x.astype(bf16).astype(f32)
        low = (ids >= pairs) & (ids < 2 * pairs)
        return jnp.where(low, x - hi, hi).astype(bf16)

    def body(m, carry):
        both = jnp.dot(gy_ref[m], dens_ref[...], preferred_element_type=f32)
        lhs = mixed(jnp.concatenate([both[:rows], both[rows:]], axis=1))
        back = []
        for j in range(columns):
            cols = lhs[:, j * WIDE:(j + 1) * WIDE]
            pts_ref[j] = jnp.dot(pw_ref[...], cols, preferred_element_type=f32)
            for g in range(0, grid_points, step):
                part = pl.ds(g, step)
                p = pts_ref[j, part, :] + core_ref[part, :]
                u = p * p + 0.25
                v = jnp.exp2(jnp.log(u) * (-1.0 / (6.0 * math.log(2.0))))
                r = v / (7.8 + C_RS * v)
                v2 = v * v
                br = 0.44 * r
                eacc_ref[j, part, :] += (u * v2) * (EX_A + br)
                pot = (p * v2) * (EX_D + (0.44 + (0.44 * C_RS / 3.0) * r) * r)
                hi = pot.astype(bf16)
                hi_ref[j, part, :] = hi
                lo_ref[j, part, :] = (pot - hi.astype(f32)).astype(bf16)
            first = jnp.dot(pwb_ref[...], hi_ref[j], preferred_element_type=f32)
            second = jnp.dot(pwb_ref[:rows, :], lo_ref[j], preferred_element_type=f32)
            back.append(first[:rows] + first[rows:] + second)
        back = mixed(jnp.concatenate(back, axis=1))
        start = pl.multiple_of(m * 2 * rows, 2 * rows)
        back_ref[pl.ds(start, rows), :] = back[:, :atoms]
        back_ref[pl.ds(start + rows, rows), :] = back[:, atoms:]
        return carry

    lax.fori_loop(0, couples, body, 0)
    ham = jnp.dot(gyb_ref[...], back_ref[...], preferred_element_type=f32)
    sums = [
        jnp.sum(eacc_ref[j] * weight_ref[...], axis=0, keepdims=True) for j in range(columns)
    ]
    sums = jnp.concatenate(sums, axis=1)
    energy = -(sums[:, :atoms] + sums[:, atoms:])
    ids = lax.broadcasted_iota(jnp.int32, (packed, atoms), 0)
    hi, lo = two(jnp.where(ids == entries, energy, ham))
    for c, windows in enumerate(chunks):
        base = len(windows) * LANES
        tails = []
        for i, k in enumerate(windows):
            sel = sel_ref[k * half:(k + 1) * half, :]
            out = dot_last(sel, hi) + dot_last(sel, lo)
            res_ref[c, :, i * LANES:(i + 1) * LANES] = out[:, :LANES]
            tails.append(out[:, LANES:])
        if len(windows) == 1:
            tails.append(jnp.zeros((half, TAIL), f32))
            res_ref[c, :, base + LANES:] = jnp.zeros((half, LANES), f32)
        res_ref[c, :, base:base + LANES] = jnp.concatenate(tails, axis=1)

def prepare(gaunt, pair_waves, y_table, core, radial_weights):
    entries = gaunt.shape[0]
    harmonics, directions = y_table.shape
    pairs, grid_points = pair_waves.shape
    rows = round_up(3 * pairs, 16)
    extra = rows - 3 * pairs
    packed = LANES + TAIL
    assert directions % 2 == 0
    fused = jnp.einsum(
        "plq,ln->nqp", gaunt.reshape(entries, harmonics, pairs), y_table, precision=highest
    )
    fused = jnp.pad(fused, ((0, 0), (0, 0), (0, packed - entries)))
    hi, lo = split(fused)
    wide = lambda a, b, c: jnp.pad(
        jnp.concatenate([a, b, c], axis=1), ((0, 0), (0, extra), (0, 0))
    )
    hi3 = wide(hi, hi, hi)
    lo3 = wide(lo, lo, lo)
    gy = jnp.concatenate([hi3, hi3, lo3], axis=2).reshape(directions // 2, 2 * rows, 3 * packed)
    gyb = wide(hi, hi, lo).reshape(directions * rows, packed).T
    pw_hi, pw_lo = split(pair_waves)
    pw = jnp.pad(jnp.concatenate([pw_hi, pw_hi, pw_lo], axis=0), ((0, extra), (0, 0))).T
    point_weight = 4.0 * jnp.pi / directions * radial_weights
    b_hi, b_lo = split(-point_weight[None, :] * pair_waves)
    triple = lambda x: jnp.pad(jnp.concatenate([x, x, x], axis=0), ((0, extra), (0, 0)))
    pwb = jnp.concatenate([triple(b_hi), triple(b_lo)], axis=0)
    core_wide = jnp.broadcast_to(core[:, None], (grid_points, WIDE))
    weight_wide = jnp.broadcast_to(point_weight[:, None], (grid_points, WIDE))
    return gy, gyb, pw, pwb, core_wide, weight_wide

def local(memory):
    return pl.BlockSpec(memory_space=memory)

def dealt(dens_part, counts, gaunt, pair_waves, y_table, core, radial_weights):
    domains = lax.axis_size("domain")
    entries, slots = dens_part.shape[1:]
    pairs, grid_points = pair_waves.shape
    half = SUBLANES * domains
    width = 2 * half
    chunks = chunk_plan(slots, width)
    n = len(chunks)
    lanes = (len(chunks[0]) + 1) * LANES
    atoms = slots // 3 // 2
    packed = LANES + TAIL
    vmem, smem = pltpu.VMEM, pltpu.SMEM
    dma = pltpu.SemaphoreType.DMA
    own_count = jnp.broadcast_to(counts.reshape(1, 1), (SUBLANES, LANES))
    recv, every_count, perm = pl.pallas_call(
        lambda *refs: scatter_kernel(*refs, domains=domains),
        out_shape=(
            jax.ShapeDtypeStruct((n, half, lanes), f32),
            jax.ShapeDtypeStruct((domains, SUBLANES, LANES), jnp.int32),
            jax.ShapeDtypeStruct((width, width), bf16),
        ),
        in_specs=[local(vmem)] * 2,
        out_specs=(local(vmem),) * 3,
        scratch_shapes=[
            vmem((lanes, width), f32),
            vmem((n, width, lanes), f32),
            vmem((n, half, lanes), f32),
            dma((domains,)), dma((domains,)), dma((n,)), dma((n,)),
            dma((n, domains)), dma((n, domains)),
        ],
        compiler_params=pltpu.CompilerParams(
            collective_id=0, has_side_effects=True, vmem_limit_bytes=32 * 1024 * 1024
        ),
        name="scatter",
    )(dens_part[0], own_count)

    tables = prepare(gaunt, pair_waves, y_table, core, radial_weights)
    gyb = tables[1]
    columns = 2 * atoms // WIDE
    step = 80 if grid_points % 80 == 0 else grid_points
    me = (2 * lax.axis_index("domain") + lax.axis_index("band")).reshape(1).astype(jnp.int32)
    result = pl.pallas_call(
        lambda *refs: atom_kernel(
            *refs, pairs=pairs, step=step, entries=entries, domains=domains, slots=slots
        ),
        out_shape=jax.ShapeDtypeStruct((n, half, lanes), f32),
        in_specs=[local(smem)] + [local(vmem)] * 8,
        out_specs=local(vmem),
        scratch_shapes=[
            vmem((slots // 2, atoms), bf16),
            vmem((packed, slots // 2), f32),
            vmem((3 * packed, atoms), bf16),
            vmem((columns, grid_points, WIDE), f32),
            vmem((columns, grid_points, WIDE), bf16),
            vmem((columns, grid_points, WIDE), bf16),
            vmem((columns, grid_points, WIDE), f32),
            vmem((gyb.shape[1], atoms), bf16),
        ],
        compiler_params=pltpu.CompilerParams(vmem_limit_bytes=48 * 1024 * 1024),
        name="atoms",
    )(me, recv, every_count, *tables)

    ham, energy = pl.pallas_call(
        lambda *refs: gather_kernel(*refs, domains=domains),
        out_shape=(
            jax.ShapeDtypeStruct((entries, slots), f32),
            jax.ShapeDtypeStruct((1, slots), f32),
        ),
        in_specs=[local(vmem)] * 2,
        out_specs=(local(vmem),) * 2,
        scratch_shapes=[
            vmem((n, half, lanes), f32),
            vmem((n, half, lanes), f32),
            dma((n,)), dma((n,)), dma((n, domains)), dma((n, domains)),
        ],
        compiler_params=pltpu.CompilerParams(
            collective_id=1, has_side_effects=True, vmem_limit_bytes=32 * 1024 * 1024
        ),
        name="gather",
    )(result, perm)
    return ham, energy.reshape(slots)

def fits(bands, domains, entries, slots):
    workers = bands * domains
    return (
        bands == 2
        and workers & (workers - 1) == 0
        and (SUBLANES * domains) % LANES == 0
        and slots % (SUBLANES * workers) == 0
        and slots % (3 * bands * LANES) == 0
        and LANES < entries < LANES + TAIL
    )

def solution(mesh):
    bands, domains = mesh.shape["band"], mesh.shape["domain"]

    def per_device(dens_part, *rest):
        entries, slots = dens_part.shape[1:]
        path = dealt if fits(bands, domains, entries, slots) else general
        return path(dens_part, *rest)

    return jax.shard_map(
        per_device,
        mesh=mesh,
        in_specs=(P("band", None, "domain"), P("domain"), P(), P(), P(), P(), P()),
        out_specs=(P(None, "domain"), P("domain")),
        check_vma=False,
    )
```

```python
import math

import jax
import jax.numpy as jnp
from jax import lax
from jax.experimental import pallas as pl
from jax.experimental.pallas import tpu as pltpu
from jax.sharding import PartitionSpec as P

highest = lax.Precision.HIGHEST
f32 = jnp.float32
bf16 = jnp.bfloat16

LANES = 128
WIDE = 256

C_RS = 0.6203504908994
EX_A = 0.7385587663820224
EX_D = 0.9847450218426965

def round_up(value, step):
    return -(-value // step) * step

def split(x):
    hi = lax.reduce_precision(x, 8, 7)
    return hi.astype(bf16), (x - hi).astype(bf16)

def general_kernel(
    dens_ref, gy_ref, gyb_ref, pw_ref, pwb_ref, core_ref, weight_ref,
    ham_ref, energy_ref, pts_ref, hi_ref, lo_ref, eacc_ref, back_ref, *, pairs, step
):
    atoms = dens_ref.shape[1]
    rows = pw_ref.shape[1]
    grid_points = pw_ref.shape[0]
    couples = gy_ref.shape[0]
    chunks = 2 * atoms // WIDE
    eacc_ref[...] = jnp.zeros_like(eacc_ref)

    def mixed(x):
        ids = lax.broadcasted_iota(jnp.int32, x.shape, 0)
        hi = x.astype(bf16).astype(f32)
        low = (ids >= pairs) & (ids < 2 * pairs)
        return jnp.where(low, x - hi, hi).astype(bf16)

    def body(m, carry):
        both = jnp.dot(gy_ref[m], dens_ref[...], preferred_element_type=f32)
        lhs = mixed(jnp.concatenate([both[:rows], both[rows:]], axis=1))
        back = []
        for j in range(chunks):
            cols = lhs[:, j * WIDE:(j + 1) * WIDE]
            pts_ref[j] = jnp.dot(pw_ref[...], cols, preferred_element_type=f32)
            for g in range(0, grid_points, step):
                part = pl.ds(g, step)
                p = pts_ref[j, part, :] + core_ref[part, :]
                u = p * p + 0.25
                v = jnp.exp2(jnp.log(u) * (-1.0 / (6.0 * math.log(2.0))))
                r = v / (7.8 + C_RS * v)
                v2 = v * v
                br = 0.44 * r
                eacc_ref[j, part, :] += (u * v2) * (EX_A + br)
                pot = (p * v2) * (EX_D + (0.44 + (0.44 * C_RS / 3.0) * r) * r)
                hi = pot.astype(bf16)
                hi_ref[j, part, :] = hi
                lo_ref[j, part, :] = (pot - hi.astype(f32)).astype(bf16)
            first = jnp.dot(pwb_ref[...], hi_ref[j], preferred_element_type=f32)
            second = jnp.dot(pwb_ref[:rows, :], lo_ref[j], preferred_element_type=f32)
            back.append(first[:rows] + first[rows:] + second)
        back = mixed(jnp.concatenate(back, axis=1))
        start = pl.multiple_of(m * 2 * rows, 2 * rows)
        back_ref[pl.ds(start, rows), :] = back[:, :atoms]
        back_ref[pl.ds(start + rows, rows), :] = back[:, atoms:]
        return carry

    lax.fori_loop(0, couples, body, 0)
    ham_ref[...] = jnp.dot(gyb_ref[...], back_ref[...], preferred_element_type=f32)
    sums = [
        jnp.sum(eacc_ref[j] * weight_ref[...], axis=0, keepdims=True) for j in range(chunks)
    ]
    sums = jnp.concatenate(sums, axis=1)
    energy_ref[...] = jnp.broadcast_to(
        -(sums[:, :atoms] + sums[:, atoms:]), energy_ref.shape
    )

def general_tables(gaunt, pair_waves, y_table, core, radial_weights):
    entries = gaunt.shape[0]
    harmonics, directions = y_table.shape
    pairs, grid_points = pair_waves.shape
    rows = round_up(3 * pairs, 16)
    extra = rows - 3 * pairs
    assert directions % 2 == 0
    fused = jnp.einsum(
        "plq,ln->nqp", gaunt.reshape(entries, harmonics, pairs), y_table, precision=highest
    )

    hi, lo = split(fused)
    wide = lambda a, b, c: jnp.pad(
        jnp.concatenate([a, b, c], axis=1), ((0, 0), (0, extra), (0, 0))
    )
    hi3 = wide(hi, hi, hi)
    lo3 = wide(lo, lo, lo)
    gy = jnp.concatenate([hi3, hi3, lo3], axis=2).reshape(directions // 2, 2 * rows, 3 * entries)
    gyb = wide(hi, hi, lo).reshape(directions * rows, entries).T
    pw_hi, pw_lo = split(pair_waves)
    pw = jnp.pad(jnp.concatenate([pw_hi, pw_hi, pw_lo], axis=0), ((0, extra), (0, 0))).T
    point_weight = 4.0 * jnp.pi / directions * radial_weights
    b_hi, b_lo = split(-point_weight[None, :] * pair_waves)
    triple = lambda x: jnp.pad(jnp.concatenate([x, x, x], axis=0), ((0, extra), (0, 0)))
    pwb = jnp.concatenate([triple(b_hi), triple(b_lo)], axis=0)
    core_wide = jnp.broadcast_to(core[:, None], (grid_points, WIDE))
    weight_wide = jnp.broadcast_to(point_weight[:, None], (grid_points, WIDE))
    return gy, gyb, pw, pwb, core_wide, weight_wide

def general_energy(columns, tables, pairs):
    entries, atoms = columns.shape
    gy, gyb, pw, pwb, core_wide, weight_wide = tables
    grid_points, rows = pw.shape
    hi, lo = split(columns)
    dens = jnp.concatenate([hi, lo, hi], axis=0)
    chunks = 2 * atoms // WIDE
    step = 80 if grid_points % 80 == 0 else grid_points

    ham, energy = pl.pallas_call(
        lambda *refs: general_kernel(*refs, pairs=pairs, step=step),
        out_shape=(
            jax.ShapeDtypeStruct((entries, atoms), f32),
            jax.ShapeDtypeStruct((8, atoms), f32),
        ),
        scratch_shapes=[
            pltpu.VMEM((chunks, grid_points, WIDE), f32),
            pltpu.VMEM((chunks, grid_points, WIDE), bf16),
            pltpu.VMEM((chunks, grid_points, WIDE), bf16),
            pltpu.VMEM((chunks, grid_points, WIDE), f32),
            pltpu.VMEM((gyb.shape[1], atoms), bf16),
        ],
        compiler_params=pltpu.CompilerParams(vmem_limit_bytes=48 * 1024 * 1024),
        name="atoms",
    )(dens, gy, gyb, pw, pwb, core_wide, weight_wide)
    return ham, energy[:1]

def general(dens_part, counts, gaunt, pair_waves, y_table, core, radial_weights):
    band_count = lax.axis_size("band")
    domain_count = lax.axis_size("domain")
    workers = band_count * domain_count
    axes = ("domain", "band")
    me = lax.axis_index("domain") * band_count + lax.axis_index("band")
    entries = dens_part.shape[1]
    slot_total = dens_part.shape[2]
    share = slot_total // band_count
    capacity = -(-share // workers)
    worker_rows = -(-(slot_total // 3) // band_count)
    atoms = round_up(worker_rows, LANES)
    tables = general_tables(gaunt, pair_waves, y_table, core, radial_weights)

    own_cols = lax.psum_scatter(dens_part[0], "band", scatter_dimension=1, tiled=True)
    every_count = lax.all_gather(counts, "domain", axis=0, tiled=True)
    band_ids = jnp.arange(band_count, dtype=jnp.int32)
    live = jnp.clip(every_count[:, None] - band_ids[None, :] * share, 0, share).reshape(-1)
    ids = jnp.arange(workers, dtype=jnp.int32)
    starts = jnp.sum(jnp.where(ids[None, :] < ids[:, None], live[None, :], 0), axis=1)
    ends = starts + live
    own_start = jnp.sum(jnp.where(ids == me, starts, 0))
    own_live = jnp.sum(jnp.where(ids == me, live, 0))
    is_alive = jnp.arange(share, dtype=jnp.int32) < own_live

    own_cols = jnp.where(is_alive[None, :], own_cols, 0.0)
    own_cols = jnp.pad(own_cols, ((0, 0), (0, capacity * workers - share)))
    blocks = own_cols.T.reshape(capacity, workers, entries).transpose(1, 0, 2)
    outgoing = jnp.roll(blocks, own_start % workers, axis=0)
    incoming = lax.all_to_all(outgoing, axes, split_axis=0, concat_axis=0, tiled=True)

    atom_ids = jnp.arange(atoms, dtype=jnp.int32) * workers + me
    source = jnp.sum((ends[None, :] <= atom_ids[:, None]).astype(jnp.int32), axis=1)
    source = jnp.minimum(source, workers - 1)
    source_start = jnp.sum(jnp.where(source[:, None] == ids[None, :], starts[None, :], 0), axis=1)
    position = jnp.clip((atom_ids - source_start) // workers, 0, capacity - 1)
    compact = jnp.take(
        incoming.reshape(workers * capacity, entries), source * capacity + position, axis=0,
        mode="clip",
    )
    ham, energy = general_energy(compact.T, tables, pair_waves.shape[0])
    result = jnp.concatenate([ham, energy], axis=0).T
    row = (me - starts) % workers
    first = (starts + row - me) // workers
    target = first[:, None] + jnp.arange(capacity, dtype=jnp.int32)[None, :]
    back = jnp.take(result, jnp.clip(target, 0, atoms - 1).reshape(-1), axis=0, mode="clip")
    returned = lax.all_to_all(
        back.reshape(workers, capacity, entries + 1), axes, split_axis=0, concat_axis=0, tiled=True
    )
    returned = jnp.roll(returned, -(own_start % workers), axis=0)
    piece = returned.transpose(1, 0, 2).reshape(capacity * workers, entries + 1)[:share]
    piece = jnp.where(is_alive[:, None], piece, 0.0)
    band = lax.axis_index("band")
    whole = jnp.zeros((slot_total, entries + 1), f32)
    ring = [(i, (i + 1) % band_count) for i in range(band_count)]
    for hop in range(band_count):
        owner = (band - hop) % band_count
        whole = lax.dynamic_update_slice(whole, piece, (owner * share, 0))
        if hop + 1 < band_count:
            piece = lax.ppermute(piece, "band", ring)
    whole = whole.T
    return whole[:entries], whole[entries]

MESH = pl.DeviceIdType.MESH
SUBLANES = 8
TAIL = 64
STEP = 80
E1 = 0.44 / 7.8
E2 = 0.44 * C_RS / (3.0 * 7.8 * 7.8)

def chunk_plan(slots, width, odd_first):
    windows = slots // width
    lead = windows % 2 if odd_first else 0
    pieces = [range(lead)] if lead else []
    return pieces + [range(k, min(k + 2, windows)) for k in range(lead, windows, 2)]

def dot_last(a, b):
    return lax.dot_general(a, b, (((1,), (1,)), ((), ())), preferred_element_type=f32)

def two(x):
    hi = x.astype(bf16)
    return hi, (x - hi.astype(f32)).astype(bf16)

def greet(domains, domain, band):
    barrier = pltpu.get_barrier_semaphore()

    def hello(off, carry):
        peer = lax.rem(domain + off, domains)
        pl.semaphore_signal(barrier, inc=1, device_id=(band, peer), device_id_type=MESH)
        return carry

    lax.fori_loop(1, domains, hello, 0)
    pl.semaphore_signal(barrier, inc=1, device_id=(1 - band, domain), device_id_type=MESH)
    pl.semaphore_wait(barrier, domains)

def whole_kernel(
    dens_ref, cnt_ref, gaunt_ref, waves_ref, y_ref, core_ref, radial_ref,
    ham_ref, energy_ref,
    own_ref, all_ref, perm_ref, stage, send, cross, recv, res_ref, got, cross_back,
    sel_ref, stack_ref, gpad_ref, ypad_ref, wpad_ref, coef_ref, flow_ref, back_ref,
    pts_ref, hi_ref, lo_ref, eacc_ref, outs_ref,
    cnt_out, cnt_in, x_out, x_in, a_out, a_in, rx_out, rx_in, ra_out, ra_in,
    *, step, domains, depth_of
):
    band, domain = lax.axis_index("band"), lax.axis_index("domain")
    entries, slots = dens_ref.shape[1:]
    fields = gaunt_ref.shape[1]
    pairs, grid_points = waves_ref.shape
    harmonics, directions = y_ref.shape
    workers = 2 * domains
    half = SUBLANES * domains
    width = 2 * half
    windows_all = slots // width
    outward = chunk_plan(slots, width, True)
    homeward = chunk_plan(slots, width, False)
    extra = entries - LANES
    atoms = sel_ref.shape[1]
    tiles = atoms // LANES
    qp, lp, np_ = round_up(pairs, 8), round_up(harmonics, 16), round_up(directions, 8)
    nn = round_up(directions, 16)
    depth = 3 * qp + 8
    packed = LANES + TAIL
    couples = directions // 2
    mine = pl.ds(pl.multiple_of(domain * SUBLANES, SUBLANES), SUBLANES)

    def loop(first, function):
        def turn(off, carry):
            function(off)
            return carry
        lax.fori_loop(first, domains, turn, 0)

    def lanes_of(windows):
        return (len(windows) + 1) * LANES

    def count_copy(off):
        peer = lax.rem(domain + off, domains)
        return pltpu.make_async_remote_copy(
            src_ref=own_ref, dst_ref=all_ref.at[domain], send_sem=cnt_out.at[off],
            recv_sem=cnt_in.at[off], device_id=(band, peer), device_id_type=MESH,
        )

    def pair_copy(source, target, c, windows, out_sem, in_sem, first):
        lanes = pl.ds(0, lanes_of(windows))
        return pltpu.make_async_remote_copy(
            src_ref=source.at[c, pl.ds(first, half), lanes],
            dst_ref=target.at[c, :, lanes], send_sem=out_sem.at[c],
            recv_sem=in_sem.at[c], device_id=(1 - band, domain), device_id_type=MESH,
        )

    def plane_copy(source, target, c, windows, out_sem, in_sem, off):
        lanes = pl.ds(0, lanes_of(windows))
        peer = lax.rem(domain + off, domains)
        rows = pl.ds(pl.multiple_of(peer * SUBLANES, SUBLANES), SUBLANES)
        return pltpu.make_async_remote_copy(
            src_ref=source.at[c, rows, lanes],
            dst_ref=target.at[c, mine, lanes], send_sem=out_sem.at[c, off],
            recv_sem=in_sem.at[c, off], device_id=(band, peer), device_id_type=MESH,
        )

    def sum_copy(c):
        return pair_copy(send, cross, c, outward[c], x_out, x_in, half)

    def deal_copy(c, off):
        return plane_copy(send, recv, c, outward[c], a_out, a_in, off)

    def back_copy(c, off):
        return plane_copy(res_ref, got, c, homeward[c], ra_out, ra_in, off)

    def share_copy(c):
        return pair_copy(got, cross_back, c, homeward[c], rx_out, rx_in, 0)

    greet(domains, domain, band)
    own_ref[...] = jnp.full((SUBLANES, LANES), cnt_ref[0], jnp.int32)
    loop(1, lambda off: count_copy(off).start())
    all_ref[domain] = own_ref[...]
    stage[...] = jnp.zeros_like(stage)
    hi_ref[...] = jnp.zeros_like(hi_ref)
    lo_ref[...] = jnp.zeros_like(lo_ref)
    back_ref[...] = jnp.zeros_like(back_ref)
    flow_ref[...] = jnp.zeros_like(flow_ref)
    gpad_ref[...] = jnp.zeros_like(gpad_ref)
    ypad_ref[...] = jnp.zeros_like(ypad_ref)
    wpad_ref[...] = jnp.zeros_like(wpad_ref)
    loop(1, lambda off: count_copy(off).wait_recv())
    start = jnp.zeros((SUBLANES, LANES), jnp.int32)
    for d in range(domains):
        start = start + jnp.where(d < domain, all_ref[d], 0)
    start = start[:1, :1]
    row = lax.broadcasted_iota(jnp.int32, (width, width), 0)
    slot = lax.broadcasted_iota(jnp.int32, (width, width), 1)
    own = row < half
    row = jnp.where(own, row, row - half)
    worker = 2 * (row // SUBLANES) + jnp.where(own, band, 1 - band)
    source = ((worker - start) & (workers - 1)) + workers * (row % SUBLANES)
    perm = jnp.where(slot == source, 1.0, 0.0).astype(bf16)
    perm_ref[...] = perm
    for c, windows in enumerate(outward):
        base = len(windows) * LANES
        for i, k in enumerate(windows):
            part = pl.ds(k * width, width)
            stage[i * LANES:(i + 1) * LANES, :] = dens_ref[0, :LANES, part]
            stage[base + i * TAIL:base + i * TAIL + extra, :] = dens_ref[0, LANES:, part]
            rest = slice(base + i * TAIL + extra, base + (i + 1) * TAIL)
            stage[rest, :] = jnp.zeros((TAIL - extra, width), f32)
        if len(windows) == 1:
            stage[base + TAIL:base + 2 * TAIL, :] = jnp.zeros((TAIL, width), f32)
        hi, lo = two(stage[:base + LANES, :])
        send[c, :, :base + LANES] = dot_last(perm, hi) + dot_last(perm, lo)
        sum_copy(c).start()

    def product(a_hi, a_lo, x):
        x_hi, x_lo = two(x)
        return (
            jnp.dot(a_hi, x_hi, preferred_element_type=f32)
            + jnp.dot(a_hi, x_lo, preferred_element_type=f32)
            + jnp.dot(a_lo, x_hi, preferred_element_type=f32)
        )

    gpad_ref[:entries, :] = gaunt_ref[...]
    r = lax.broadcasted_iota(jnp.int32, (pairs * lp, fields), 0)
    col = lax.broadcasted_iota(jnp.int32, (pairs * lp, fields), 1)
    wanted = jnp.where(r % lp < harmonics, (r % lp) * pairs + r // lp, -1)
    order = jnp.where(wanted == col, 1.0, 0.0).astype(bf16)
    g_hi, g_lo = two(gpad_ref[...])
    into_hi, into_lo = dot_last(order, g_hi).astype(bf16), dot_last(order, g_lo).astype(bf16)
    out_hi, out_lo = dot_last(g_hi, order).astype(bf16), dot_last(g_lo, order).astype(bf16)
    ypad_ref[:harmonics, :directions] = y_ref[...]
    y_hi, y_lo = two(ypad_ref[...])
    turned = ypad_ref[...].T[:nn, :lp]
    yt_hi, yt_lo = two(turned)

    point_weight = (4.0 * math.pi / directions) * radial_ref[...]
    waves = waves_ref[...]
    waves_hi = waves.astype(bf16).astype(f32)
    core = core_ref[...]
    core_hi = core.astype(bf16).astype(f32)
    core_mid = (core - core_hi).astype(bf16).astype(f32)
    wpad_ref[:pairs, :grid_points] = waves_hi
    wpad_ref[qp:qp + pairs, :grid_points] = waves_hi
    wpad_ref[2 * qp:2 * qp + pairs, :grid_points] = waves - waves_hi
    wpad_ref[3 * qp:3 * qp + 1, :grid_points] = core_hi
    wpad_ref[3 * qp + 1:3 * qp + 2, :grid_points] = core_mid
    wpad_ref[3 * qp + 2:3 * qp + 3, :grid_points] = core - core_hi - core_mid
    wpad_ref[depth:depth + 1, :grid_points] = point_weight
    turned = wpad_ref[...].T
    forward = turned[:grid_points, :depth].astype(bf16)
    weight = turned[:grid_points, depth:depth + 1]
    wpad_ref[:qp, :] = jnp.zeros((qp, wpad_ref.shape[1]), f32)
    wpad_ref[:pairs, :grid_points] = waves * (-E2 * point_weight)
    b_hi, b_lo = two(wpad_ref[:qp, :grid_points])
    reverse = jnp.concatenate([b_hi.astype(f32), b_lo.astype(f32)], axis=0).astype(bf16)

    me = 2 * domain + band
    row = lax.broadcasted_iota(jnp.int32, (half, LANES), 0)
    held, begun = [], jnp.zeros((1, LANES), jnp.int32)
    for d in range(domains):
        value = all_ref[d][:1, :]
        held.append(jnp.maximum((value - ((me - begun) & (workers - 1)) + workers - 1) // workers, 0))
        begun = begun + value
    lane = lax.broadcasted_iota(jnp.int32, (half, atoms), 1)
    base = jnp.zeros((1, LANES), jnp.int32)
    for k in range(windows_all):
        rank = jnp.zeros((half, LANES), jnp.int32) + row % SUBLANES + base
        live = jnp.zeros((half, LANES), jnp.int32)
        for d in range(domains):
            here = jnp.clip(held[d] - SUBLANES * k, 0, SUBLANES)
            rank = rank + jnp.where(row >= (d + 1) * SUBLANES, here, 0)
            live = jnp.where(row // SUBLANES == d, here, live)
            base = base + here
        rank = jnp.where(row % SUBLANES < live, rank, -1)
        rank = jnp.concatenate([rank] * tiles, axis=1)
        sel_ref[k * half:(k + 1) * half, :] = jnp.where(rank == lane, 1.0, 0.0).astype(bf16)

    def deal(c):
        lanes = lanes_of(outward[c])
        sum_copy(c).wait_recv()
        send[c, :half, :lanes] += cross[c, :, :lanes]
        loop(1, lambda off: deal_copy(c, off).start())
        recv[c, mine, :lanes] = send[c, mine, :lanes]

    def take(c):
        loop(1, lambda off: deal_copy(c, off).wait_recv())
        windows = outward[c]
        base = len(windows) * LANES
        tails = recv[c, :, base:base + LANES].T
        for i, k in enumerate(windows):
            spot = slice(k * half, (k + 1) * half)
            stack_ref[:LANES, spot] = recv[c, :, i * LANES:(i + 1) * LANES].T
            stack_ref[LANES:, spot] = tails[i * TAIL:(i + 1) * TAIL]

    def give(c, known):
        windows = homeward[c]
        base = len(windows) * LANES
        span = slice(0, known * LANES)
        tails = []
        for i, k in enumerate(windows):
            sel = sel_ref[k * half:(k + 1) * half, span]
            out = dot_last(sel, outs_ref[0, :, span]) + dot_last(sel, outs_ref[1, :, span])
            res_ref[c, :, i * LANES:(i + 1) * LANES] = out[:, :LANES]
            tails.append(out[:, LANES:])
        if len(windows) == 1:
            tails.append(jnp.zeros((half, TAIL), f32))
        res_ref[c, :, base:base + LANES] = jnp.concatenate(tails, axis=1)
        loop(1, lambda off: back_copy(c, off).start())
        got[c, mine, :base + LANES] = res_ref[c, mine, :base + LANES]

    def share(c):
        loop(1, lambda off: back_copy(c, off).wait_recv())
        share_copy(c).start()

    def places(n):
        return [pl.ds(2 * n + i, qp, stride=np_) for i in range(2)]

    ones = jnp.ones((8, WIDE), f32)

    def enter(n, s):
        x = jnp.concatenate([flow_ref[at, :] for at in places(n)], axis=1)
        hi = x.astype(bf16).astype(f32)
        cols = jnp.concatenate([hi, x - hi, hi, ones], axis=0).astype(bf16)
        pts_ref[s] = jnp.dot(forward, cols, preferred_element_type=f32)

    def leave(n, s):
        both = jnp.dot(reverse, hi_ref[s], preferred_element_type=f32)
        out = both[:qp] + both[qp:] + jnp.dot(b_hi, lo_ref[s], preferred_element_type=f32)
        for i, at in enumerate(places(n)):
            back_ref[at, :] = out[:, i * LANES:(i + 1) * LANES]

    def evaluate(s):
        for g in range(0, grid_points, step):
            part = pl.ds(g, step)
            p = pts_ref[s, part, :]
            u = p * p + 0.25
            power = jnp.log2(u)
            t = jnp.exp2(power * (1.0 / 6.0))
            w = jnp.exp2(power * (-1.0 / 3.0))
            r = 1.0 / (t + C_RS / 7.8)
            eacc_ref[s, part, :] += (u * w) * (r + EX_A / E1)
            pot = (p * w) * ((r + E1 / E2) * r + EX_D / E2)
            hi = pot.astype(bf16)
            hi_ref[s, part, :] = hi
            lo_ref[s, part, :] = (pot - hi.astype(f32)).astype(bf16)

    def compute(i, services):
        rows = slice(0, -(-(i + 1) * windows_all // tiles) * half)
        span = slice(i * LANES, (i + 1) * LANES)
        sel = sel_ref[rows, span]
        hi, lo = two(stack_ref[:, rows])
        hi = jnp.dot(hi, sel, preferred_element_type=f32).astype(bf16)
        lo = jnp.dot(lo, sel, preferred_element_type=f32).astype(bf16)
        coef_ref[...] = (
            jnp.dot(into_hi, hi, preferred_element_type=f32)
            + jnp.dot(into_hi, lo, preferred_element_type=f32)
            + jnp.dot(into_lo, hi, preferred_element_type=f32)
        )
        for q in range(pairs):
            flow = product(yt_hi, yt_lo, coef_ref[q * lp:(q + 1) * lp, :])
            flow_ref[q * np_:(q + 1) * np_, :] = flow[:np_]
        eacc_ref[...] = jnp.zeros_like(eacc_ref)
        enter(0, 0)

        def body(turn, carry):
            for at, service in services:
                @pl.when(turn == at)
                def _():
                    service()
            for s in range(depth_of):
                n = turn * depth_of + s
                enter(jnp.minimum(n + 1, couples - 1), (s + 1) % depth_of)
                leave(jnp.maximum(n - 1, 0), (s - 1) % depth_of)
                evaluate(s)
            return carry

        lax.fori_loop(0, couples // depth_of, body, 0)
        leave(couples - 1, depth_of - 1)
        for q in range(pairs):
            coef_ref[q * lp:(q + 1) * lp, :] = product(
                y_hi[:lp, :np_], y_lo[:lp, :np_], back_ref[q * np_:(q + 1) * np_, :]
            )
        ham = product(out_hi, out_lo, coef_ref[...])
        total = eacc_ref[0]
        for s in range(1, depth_of):
            total = total + eacc_ref[s]
        total = jnp.sum(total * weight, axis=0, keepdims=True)
        energy = -E1 * (total[:, :LANES] + total[:, LANES:])
        ids = lax.broadcasted_iota(jnp.int32, (packed, LANES), 0)
        hi, lo = two(jnp.where(ids == entries, energy, ham))
        outs_ref[0, :, span] = hi
        outs_ref[1, :, span] = lo

    def last_needed(i):
        need = -(-(i + 1) * windows_all // tiles)
        return next(c for c, windows in enumerate(outward) if windows[-1] + 1 >= need)

    turns = couples // depth_of
    dealt_to, taken, given, shared = 0, 0, 0, 0
    for i in range(tiles):
        last = last_needed(i)
        while dealt_to <= last:
            deal(dealt_to)
            dealt_to += 1
        if i == 0 and dealt_to < len(outward):
            deal(dealt_to)
            dealt_to += 1
        while taken <= last:
            take(taken)
            taken += 1
        services = []
        if i == 0:
            for c in range(dealt_to, len(outward)):
                spot = min(turns - 1, 1 + 2 * (c - dealt_to))
                services.append((spot, lambda c=c: deal(c)))
            dealt_to = len(outward)
        for c in range(shared, given):
            services.append((min(turns - 1, 3), lambda c=c: share(c)))
        shared = given
        compute(i, services)
        while given < len(homeward):
            need = -(-half * (homeward[given][-1] + 1) // LANES)
            if min(need, tiles) > i + 1:
                break
            give(given, min(need, tiles))
            given += 1

    perm = perm_ref[...]

    def finish(c):
        share_copy(c).wait_recv()
        windows = homeward[c]
        base = len(windows) * LANES

        def spread(lanes):
            rows = jnp.concatenate([got[c, :, lanes], cross_back[c, :, lanes]], axis=0).T
            hi, lo = two(rows)
            return jnp.dot(hi, perm, preferred_element_type=f32) + jnp.dot(
                lo, perm, preferred_element_type=f32
            )

        tails = spread(slice(base, base + LANES))
        for i, k in enumerate(windows):
            part = pl.ds(k * width, width)
            ham_ref[:LANES, part] = spread(slice(i * LANES, (i + 1) * LANES))
            ham_ref[LANES:, part] = tails[i * TAIL:i * TAIL + extra]
            for j in range(width // LANES):
                line = k * (width // LANES) + j
                energy_ref[line:line + 1, :] = tails[
                    i * TAIL + extra:i * TAIL + extra + 1, j * LANES:(j + 1) * LANES
                ]

    finished = 0
    for c in range(shared, len(homeward)):
        share(c)
        if c:
            finish(finished)
            finished += 1
    while finished < len(homeward):
        finish(finished)
        finished += 1
    for c in range(len(outward)):
        loop(1, lambda off: deal_copy(c, off).wait_send())
        sum_copy(c).wait_send()
    for c in range(len(homeward)):
        loop(1, lambda off: back_copy(c, off).wait_send())
        share_copy(c).wait_send()
    loop(1, lambda off: count_copy(off).wait_send())

def local(memory):
    return pl.BlockSpec(memory_space=memory)

def dealt(dens_part, counts, gaunt, pair_waves, y_table, core, radial_weights):
    domains = lax.axis_size("domain")
    entries, slots = dens_part.shape[1:]
    pairs, grid_points = pair_waves.shape
    harmonics, directions = y_table.shape
    half = SUBLANES * domains
    width = 2 * half
    n = len(chunk_plan(slots, width, True))
    lanes = 3 * LANES
    atoms = slots // 3 // 2
    packed = LANES + TAIL
    vmem, smem = pltpu.VMEM, pltpu.SMEM
    dma = pltpu.SemaphoreType.DMA
    step = next(size for size in (STEP, 16, 8) if grid_points % size == 0)
    depth_of = next(size for size in (5, 4, 3, 2, 1) if directions // 2 % size == 0)
    qp, lp = round_up(pairs, 8), round_up(harmonics, 16)
    np_ = round_up(directions, 8)
    ham, energy = pl.pallas_call(
        lambda *refs: whole_kernel(*refs, step=step, domains=domains, depth_of=depth_of),
        out_shape=(
            jax.ShapeDtypeStruct((entries, slots), f32),
            jax.ShapeDtypeStruct((slots // LANES, LANES), f32),
        ),
        in_specs=[local(vmem), local(smem)] + [local(vmem)] * 5,
        out_specs=(local(vmem),) * 2,
        scratch_shapes=[
            vmem((SUBLANES, LANES), jnp.int32),
            vmem((domains, SUBLANES, LANES), jnp.int32),
            vmem((width, width), bf16),
            vmem((lanes, width), f32),
            vmem((n, width, lanes), f32),
            vmem((n, half, lanes), f32),
            vmem((n, half, lanes), f32),
            vmem((n, half, lanes), f32),
            vmem((n, half, lanes), f32),
            vmem((n, half, lanes), f32),
            vmem((slots // 2, atoms), bf16),
            vmem((packed, slots // 2), f32),
            vmem((packed, gaunt.shape[1]), f32),
            vmem((LANES, LANES), f32),
            vmem((LANES, round_up(grid_points, LANES)), f32),
            vmem((pairs * lp, LANES), f32),
            vmem((qp * np_, LANES), f32),
            vmem((qp * np_, LANES), f32),
            vmem((depth_of, grid_points, WIDE), f32),
            vmem((depth_of, grid_points, WIDE), bf16),
            vmem((depth_of, grid_points, WIDE), bf16),
            vmem((depth_of, grid_points, WIDE), f32),
            vmem((2, packed, atoms), bf16),
            dma((domains,)), dma((domains,)), dma((n,)), dma((n,)),
            dma((n, domains)), dma((n, domains)), dma((n,)), dma((n,)),
            dma((n, domains)), dma((n, domains)),
        ],
        compiler_params=pltpu.CompilerParams(
            collective_id=0, has_side_effects=True, vmem_limit_bytes=48 * 1024 * 1024
        ),
        name="whole",
    )(
        dens_part, counts, gaunt, pair_waves, y_table, core.reshape(1, grid_points),
        radial_weights.reshape(1, grid_points),
    )
    return ham, energy.reshape(slots)

def fits(bands, domains, entries, slots, pairs, grid_points, harmonics, directions):
    workers = bands * domains
    return (
        bands == 2
        and workers & (workers - 1) == 0
        and (SUBLANES * domains) % LANES == 0
        and slots % (SUBLANES * workers) == 0
        and slots % (3 * bands * LANES) == 0
        and LANES < entries < LANES + TAIL
        and directions % 2 == 0
        and max(harmonics, directions, 3 * pairs + 40) <= LANES
        and grid_points % SUBLANES == 0
    )

def solution(mesh):
    bands, domains = mesh.shape["band"], mesh.shape["domain"]

    def per_device(*arrays):
        entries, slots = arrays[0].shape[1:]
        sizes = arrays[3].shape + arrays[4].shape
        path = dealt if fits(bands, domains, entries, slots, *sizes) else general
        return path(*arrays)

    return jax.shard_map(
        per_device,
        mesh=mesh,
        in_specs=(P("band", None, "domain"), P("domain"), P(), P(), P(), P(), P()),
        out_specs=(P(None, "domain"), P("domain")),
        check_vma=False,
    )
```

```python
import math

import jax
import jax.numpy as jnp
from jax import lax
from jax.experimental import pallas as pl
from jax.experimental.pallas import tpu as pltpu
from jax.sharding import PartitionSpec as P

highest = lax.Precision.HIGHEST
f32 = jnp.float32
bf16 = jnp.bfloat16

LANES = 128
WIDE = 256

C_RS = 0.6203504908994
EX_A = 0.7385587663820224
EX_D = 0.9847450218426965

def round_up(value, step):
    return -(-value // step) * step

def split(x):
    hi = lax.reduce_precision(x, 8, 7)
    return hi.astype(bf16), (x - hi).astype(bf16)

def general_kernel(
    dens_ref, gy_ref, gyb_ref, pw_ref, pwb_ref, core_ref, weight_ref,
    ham_ref, energy_ref, pts_ref, hi_ref, lo_ref, eacc_ref, back_ref, *, pairs, step
):
    atoms = dens_ref.shape[1]
    rows = pw_ref.shape[1]
    grid_points = pw_ref.shape[0]
    couples = gy_ref.shape[0]
    chunks = 2 * atoms // WIDE
    eacc_ref[...] = jnp.zeros_like(eacc_ref)

    def mixed(x):
        ids = lax.broadcasted_iota(jnp.int32, x.shape, 0)
        hi = x.astype(bf16).astype(f32)
        low = (ids >= pairs) & (ids < 2 * pairs)
        return jnp.where(low, x - hi, hi).astype(bf16)

    def body(m, carry):
        both = jnp.dot(gy_ref[m], dens_ref[...], preferred_element_type=f32)
        lhs = mixed(jnp.concatenate([both[:rows], both[rows:]], axis=1))
        back = []
        for j in range(chunks):
            cols = lhs[:, j * WIDE:(j + 1) * WIDE]
            pts_ref[j] = jnp.dot(pw_ref[...], cols, preferred_element_type=f32)
            for g in range(0, grid_points, step):
                part = pl.ds(g, step)
                p = pts_ref[j, part, :] + core_ref[part, :]
                u = p * p + 0.25
                v = jnp.exp2(jnp.log(u) * (-1.0 / (6.0 * math.log(2.0))))
                r = v / (7.8 + C_RS * v)
                v2 = v * v
                br = 0.44 * r
                eacc_ref[j, part, :] += (u * v2) * (EX_A + br)
                pot = (p * v2) * (EX_D + (0.44 + (0.44 * C_RS / 3.0) * r) * r)
                hi = pot.astype(bf16)
                hi_ref[j, part, :] = hi
                lo_ref[j, part, :] = (pot - hi.astype(f32)).astype(bf16)
            first = jnp.dot(pwb_ref[...], hi_ref[j], preferred_element_type=f32)
            second = jnp.dot(pwb_ref[:rows, :], lo_ref[j], preferred_element_type=f32)
            back.append(first[:rows] + first[rows:] + second)
        back = mixed(jnp.concatenate(back, axis=1))
        start = pl.multiple_of(m * 2 * rows, 2 * rows)
        back_ref[pl.ds(start, rows), :] = back[:, :atoms]
        back_ref[pl.ds(start + rows, rows), :] = back[:, atoms:]
        return carry

    lax.fori_loop(0, couples, body, 0)
    ham_ref[...] = jnp.dot(gyb_ref[...], back_ref[...], preferred_element_type=f32)
    sums = [
        jnp.sum(eacc_ref[j] * weight_ref[...], axis=0, keepdims=True) for j in range(chunks)
    ]
    sums = jnp.concatenate(sums, axis=1)
    energy_ref[...] = jnp.broadcast_to(
        -(sums[:, :atoms] + sums[:, atoms:]), energy_ref.shape
    )

def general_tables(gaunt, pair_waves, y_table, core, radial_weights):
    entries = gaunt.shape[0]
    harmonics, directions = y_table.shape
    pairs, grid_points = pair_waves.shape
    rows = round_up(3 * pairs, 16)
    extra = rows - 3 * pairs
    assert directions % 2 == 0
    fused = jnp.einsum(
        "plq,ln->nqp", gaunt.reshape(entries, harmonics, pairs), y_table, precision=highest
    )

    hi, lo = split(fused)
    wide = lambda a, b, c: jnp.pad(
        jnp.concatenate([a, b, c], axis=1), ((0, 0), (0, extra), (0, 0))
    )
    hi3 = wide(hi, hi, hi)
    lo3 = wide(lo, lo, lo)
    gy = jnp.concatenate([hi3, hi3, lo3], axis=2).reshape(directions // 2, 2 * rows, 3 * entries)
    gyb = wide(hi, hi, lo).reshape(directions * rows, entries).T
    pw_hi, pw_lo = split(pair_waves)
    pw = jnp.pad(jnp.concatenate([pw_hi, pw_hi, pw_lo], axis=0), ((0, extra), (0, 0))).T
    point_weight = 4.0 * jnp.pi / directions * radial_weights
    b_hi, b_lo = split(-point_weight[None, :] * pair_waves)
    triple = lambda x: jnp.pad(jnp.concatenate([x, x, x], axis=0), ((0, extra), (0, 0)))
    pwb = jnp.concatenate([triple(b_hi), triple(b_lo)], axis=0)
    core_wide = jnp.broadcast_to(core[:, None], (grid_points, WIDE))
    weight_wide = jnp.broadcast_to(point_weight[:, None], (grid_points, WIDE))
    return gy, gyb, pw, pwb, core_wide, weight_wide

def general_energy(columns, tables, pairs):
    entries, atoms = columns.shape
    gy, gyb, pw, pwb, core_wide, weight_wide = tables
    grid_points, rows = pw.shape
    hi, lo = split(columns)
    dens = jnp.concatenate([hi, lo, hi], axis=0)
    chunks = 2 * atoms // WIDE
    step = 80 if grid_points % 80 == 0 else grid_points

    ham, energy = pl.pallas_call(
        lambda *refs: general_kernel(*refs, pairs=pairs, step=step),
        out_shape=(
            jax.ShapeDtypeStruct((entries, atoms), f32),
            jax.ShapeDtypeStruct((8, atoms), f32),
        ),
        scratch_shapes=[
            pltpu.VMEM((chunks, grid_points, WIDE), f32),
            pltpu.VMEM((chunks, grid_points, WIDE), bf16),
            pltpu.VMEM((chunks, grid_points, WIDE), bf16),
            pltpu.VMEM((chunks, grid_points, WIDE), f32),
            pltpu.VMEM((gyb.shape[1], atoms), bf16),
        ],
        compiler_params=pltpu.CompilerParams(vmem_limit_bytes=48 * 1024 * 1024),
        name="atoms",
    )(dens, gy, gyb, pw, pwb, core_wide, weight_wide)
    return ham, energy[:1]

def general(dens_part, counts, gaunt, pair_waves, y_table, core, radial_weights):
    band_count = lax.axis_size("band")
    domain_count = lax.axis_size("domain")
    workers = band_count * domain_count
    axes = ("domain", "band")
    me = lax.axis_index("domain") * band_count + lax.axis_index("band")
    entries = dens_part.shape[1]
    slot_total = dens_part.shape[2]
    share = slot_total // band_count
    capacity = -(-share // workers)
    worker_rows = -(-(slot_total // 3) // band_count)
    atoms = round_up(worker_rows, LANES)
    tables = general_tables(gaunt, pair_waves, y_table, core, radial_weights)

    own_cols = lax.psum_scatter(dens_part[0], "band", scatter_dimension=1, tiled=True)
    every_count = lax.all_gather(counts, "domain", axis=0, tiled=True)
    band_ids = jnp.arange(band_count, dtype=jnp.int32)
    live = jnp.clip(every_count[:, None] - band_ids[None, :] * share, 0, share).reshape(-1)
    ids = jnp.arange(workers, dtype=jnp.int32)
    starts = jnp.sum(jnp.where(ids[None, :] < ids[:, None], live[None, :], 0), axis=1)
    ends = starts + live
    own_start = jnp.sum(jnp.where(ids == me, starts, 0))
    own_live = jnp.sum(jnp.where(ids == me, live, 0))
    is_alive = jnp.arange(share, dtype=jnp.int32) < own_live

    own_cols = jnp.where(is_alive[None, :], own_cols, 0.0)
    own_cols = jnp.pad(own_cols, ((0, 0), (0, capacity * workers - share)))
    blocks = own_cols.T.reshape(capacity, workers, entries).transpose(1, 0, 2)
    outgoing = jnp.roll(blocks, own_start % workers, axis=0)
    incoming = lax.all_to_all(outgoing, axes, split_axis=0, concat_axis=0, tiled=True)

    atom_ids = jnp.arange(atoms, dtype=jnp.int32) * workers + me
    source = jnp.sum((ends[None, :] <= atom_ids[:, None]).astype(jnp.int32), axis=1)
    source = jnp.minimum(source, workers - 1)
    source_start = jnp.sum(jnp.where(source[:, None] == ids[None, :], starts[None, :], 0), axis=1)
    position = jnp.clip((atom_ids - source_start) // workers, 0, capacity - 1)
    compact = jnp.take(
        incoming.reshape(workers * capacity, entries), source * capacity + position, axis=0,
        mode="clip",
    )
    ham, energy = general_energy(compact.T, tables, pair_waves.shape[0])
    result = jnp.concatenate([ham, energy], axis=0).T
    row = (me - starts) % workers
    first = (starts + row - me) // workers
    target = first[:, None] + jnp.arange(capacity, dtype=jnp.int32)[None, :]
    back = jnp.take(result, jnp.clip(target, 0, atoms - 1).reshape(-1), axis=0, mode="clip")
    returned = lax.all_to_all(
        back.reshape(workers, capacity, entries + 1), axes, split_axis=0, concat_axis=0, tiled=True
    )
    returned = jnp.roll(returned, -(own_start % workers), axis=0)
    piece = returned.transpose(1, 0, 2).reshape(capacity * workers, entries + 1)[:share]
    piece = jnp.where(is_alive[:, None], piece, 0.0)
    band = lax.axis_index("band")
    whole = jnp.zeros((slot_total, entries + 1), f32)
    ring = [(i, (i + 1) % band_count) for i in range(band_count)]
    for hop in range(band_count):
        owner = (band - hop) % band_count
        whole = lax.dynamic_update_slice(whole, piece, (owner * share, 0))
        if hop + 1 < band_count:
            piece = lax.ppermute(piece, "band", ring)
    whole = whole.T
    return whole[:entries], whole[entries]

MESH = pl.DeviceIdType.MESH
SUBLANES = 8
TAIL = 64
STEP = 80
AHEAD = 2
E1 = 0.44 / 7.8
E2 = 0.44 * C_RS / (3.0 * 7.8 * 7.8)

def chunk_plan(slots, width, odd_first):
    windows = slots // width
    lead = windows % 2 if odd_first else 0
    pieces = [range(lead)] if lead else []
    return pieces + [range(k, min(k + 2, windows)) for k in range(lead, windows, 2)]

def dot_last(a, b):
    return lax.dot_general(a, b, (((1,), (1,)), ((), ())), preferred_element_type=f32)

def two(x):
    hi = x.astype(bf16)
    return hi, (x - hi.astype(f32)).astype(bf16)

def greet(domains, domain, band):
    barrier = pltpu.get_barrier_semaphore()

    def hello(off, carry):
        peer = lax.rem(domain + off, domains)
        pl.semaphore_signal(barrier, inc=1, device_id=(band, peer), device_id_type=MESH)
        return carry

    lax.fori_loop(1, domains, hello, 0)
    pl.semaphore_signal(barrier, inc=1, device_id=(1 - band, domain), device_id_type=MESH)
    pl.semaphore_wait(barrier, domains)

def whole_kernel(
    dens_ref, cnt_ref, gaunt_ref, waves_ref, y_ref, core_ref, radial_ref,
    ham_ref, energy_ref,
    own_ref, all_ref, perm_ref, stage, send, cross, recv, res_ref, got, cross_back,
    sel_ref, stack_ref, gpad_ref, ypad_ref, wpad_ref, coef_ref, flow_ref, back_ref,
    pts_ref, hi_ref, lo_ref, eacc_ref, outs_ref,
    cnt_out, cnt_in, x_out, x_in, a_out, a_in, rx_out, rx_in, ra_out, ra_in,
    *, step, domains, depth_of
):
    band, domain = lax.axis_index("band"), lax.axis_index("domain")
    entries, slots = dens_ref.shape[1:]
    fields = gaunt_ref.shape[1]
    pairs, grid_points = waves_ref.shape
    harmonics, directions = y_ref.shape
    workers = 2 * domains
    half = SUBLANES * domains
    width = 2 * half
    windows_all = slots // width
    outward = chunk_plan(slots, width, True)
    homeward = chunk_plan(slots, width, False)
    extra = entries - LANES
    atoms = sel_ref.shape[1]
    tiles = atoms // LANES
    qp, lp, np_ = round_up(pairs, 8), round_up(harmonics, 16), round_up(directions, 8)
    nn = round_up(directions, 16)
    depth = 3 * qp + 8
    packed = LANES + TAIL
    couples = directions // 2
    mine = pl.ds(pl.multiple_of(domain * SUBLANES, SUBLANES), SUBLANES)

    def loop(first, function):
        def turn(off, carry):
            function(off)
            return carry
        lax.fori_loop(first, domains, turn, 0)

    def lanes_of(windows):
        return (len(windows) + 1) * LANES

    def count_copy(off):
        peer = lax.rem(domain + off, domains)
        return pltpu.make_async_remote_copy(
            src_ref=own_ref, dst_ref=all_ref.at[domain], send_sem=cnt_out,
            recv_sem=cnt_in, device_id=(band, peer), device_id_type=MESH,
        )

    def pair_copy(source, target, c, windows, out_sem, in_sem, first):
        lanes = pl.ds(0, lanes_of(windows))
        return pltpu.make_async_remote_copy(
            src_ref=source.at[c, pl.ds(first, half), lanes],
            dst_ref=target.at[c, :, lanes], send_sem=out_sem.at[c],
            recv_sem=in_sem.at[c], device_id=(1 - band, domain), device_id_type=MESH,
        )

    def plane_copy(source, target, c, windows, out_sem, in_sem, off):
        lanes = pl.ds(0, lanes_of(windows))
        peer = lax.rem(domain + off, domains)
        rows = pl.ds(pl.multiple_of(peer * SUBLANES, SUBLANES), SUBLANES)
        return pltpu.make_async_remote_copy(
            src_ref=source.at[c, rows, lanes],
            dst_ref=target.at[c, mine, lanes], send_sem=out_sem.at[c],
            recv_sem=in_sem.at[c], device_id=(band, peer), device_id_type=MESH,
        )

    def count_all():
        others = pl.ds(0, domains - 1)
        return pltpu.make_async_remote_copy(
            src_ref=all_ref.at[others], dst_ref=all_ref.at[others], send_sem=cnt_out,
            recv_sem=cnt_in, device_id=(1 - band, domain), device_id_type=MESH,
        )

    def plane_all(source, target, c, windows, out_sem, in_sem):
        lanes = pl.ds(0, lanes_of(windows))
        rows = pl.ds(0, half - SUBLANES)
        return pltpu.make_async_remote_copy(
            src_ref=source.at[c, rows, lanes], dst_ref=target.at[c, rows, lanes],
            send_sem=out_sem.at[c], recv_sem=in_sem.at[c],
            device_id=(1 - band, domain), device_id_type=MESH,
        )

    def deal_all(c):
        return plane_all(send, recv, c, outward[c], a_out, a_in)

    def back_all(c):
        return plane_all(res_ref, got, c, homeward[c], ra_out, ra_in)

    def sum_copy(c):
        return pair_copy(send, cross, c, outward[c], x_out, x_in, half)

    def deal_copy(c, off):
        return plane_copy(send, recv, c, outward[c], a_out, a_in, off)

    def back_copy(c, off):
        return plane_copy(res_ref, got, c, homeward[c], ra_out, ra_in, off)

    def share_copy(c):
        return pair_copy(got, cross_back, c, homeward[c], rx_out, rx_in, 0)

    greet(domains, domain, band)
    own_ref[...] = jnp.full((SUBLANES, LANES), cnt_ref[0], jnp.int32)
    loop(1, lambda off: count_copy(off).start())
    all_ref[domain] = own_ref[...]
    stage[...] = jnp.zeros_like(stage)
    hi_ref[...] = jnp.zeros_like(hi_ref)
    lo_ref[...] = jnp.zeros_like(lo_ref)
    back_ref[...] = jnp.zeros_like(back_ref)
    flow_ref[...] = jnp.zeros_like(flow_ref)
    gpad_ref[...] = jnp.zeros_like(gpad_ref)
    ypad_ref[...] = jnp.zeros_like(ypad_ref)
    wpad_ref[...] = jnp.zeros_like(wpad_ref)
    count_all().wait_recv()
    start = jnp.zeros((SUBLANES, LANES), jnp.int32)
    for d in range(domains):
        start = start + jnp.where(d < domain, all_ref[d], 0)
    start = start[:1, :1]
    row = lax.broadcasted_iota(jnp.int32, (width, width), 0)
    slot = lax.broadcasted_iota(jnp.int32, (width, width), 1)
    own = row < half
    row = jnp.where(own, row, row - half)
    worker = 2 * (row // SUBLANES) + jnp.where(own, band, 1 - band)
    source = ((worker - start) & (workers - 1)) + workers * (row % SUBLANES)
    perm = jnp.where(slot == source, 1.0, 0.0).astype(bf16)
    perm_ref[...] = perm
    for c, windows in enumerate(outward):
        base = len(windows) * LANES
        for i, k in enumerate(windows):
            part = pl.ds(k * width, width)
            stage[i * LANES:(i + 1) * LANES, :] = dens_ref[0, :LANES, part]
            stage[base + i * TAIL:base + i * TAIL + extra, :] = dens_ref[0, LANES:, part]
            rest = slice(base + i * TAIL + extra, base + (i + 1) * TAIL)
            stage[rest, :] = jnp.zeros((TAIL - extra, width), f32)
        if len(windows) == 1:
            stage[base + TAIL:base + 2 * TAIL, :] = jnp.zeros((TAIL, width), f32)
        hi, lo = two(stage[:base + LANES, :])
        send[c, :, :base + LANES] = dot_last(perm, hi) + dot_last(perm, lo)
        sum_copy(c).start()

    groups = [range(q, min(q + 2, pairs)) for q in range(0, pairs, 2)]

    def side_by_side(ref, group, size):
        return jnp.concatenate([ref[q * size:(q + 1) * size, :] for q in group], axis=1)

    def terms(x):
        hi = x.astype(bf16).astype(f32)
        return jnp.concatenate([hi, x - hi, hi], axis=0).astype(bf16)

    gpad_ref[:entries, :] = gaunt_ref[...]
    r = lax.broadcasted_iota(jnp.int32, (pairs * lp, fields), 0)
    col = lax.broadcasted_iota(jnp.int32, (pairs * lp, fields), 1)
    wanted = jnp.where(r % lp < harmonics, (r % lp) * pairs + r // lp, -1)
    order = jnp.where(wanted == col, 1.0, 0.0).astype(bf16)
    g_hi, g_lo = two(gpad_ref[...])
    into_hi, into_lo = dot_last(order, g_hi).astype(bf16), dot_last(order, g_lo).astype(bf16)
    out_hi, out_lo = dot_last(g_hi, order).astype(bf16), dot_last(g_lo, order).astype(bf16)
    out_all = jnp.concatenate([out_hi, out_lo], axis=0)
    y = y_ref[...]
    near = y.astype(bf16).astype(f32)
    for i, part in enumerate((near, near, y - near)):
        ypad_ref[i * lp:i * lp + harmonics, :directions] = part
    turned = ypad_ref[...].T
    y_in = turned[:nn, :3 * lp].astype(bf16)
    blocks = [turned[:np_, i * lp:(i + 1) * lp] for i in range(3)]
    ypad_ref[...] = jnp.zeros_like(ypad_ref)
    for i, part in enumerate(blocks):
        ypad_ref[i * np_:(i + 1) * np_, :lp] = part
    y_out = ypad_ref[...].T[:lp, :3 * np_].astype(bf16)

    point_weight = (4.0 * math.pi / directions) * radial_ref[...]
    waves = waves_ref[...]
    waves_hi = waves.astype(bf16).astype(f32)
    core = core_ref[...]
    core_hi = core.astype(bf16).astype(f32)
    core_mid = (core - core_hi).astype(bf16).astype(f32)
    wpad_ref[:pairs, :grid_points] = waves_hi
    wpad_ref[qp:qp + pairs, :grid_points] = waves_hi
    wpad_ref[2 * qp:2 * qp + pairs, :grid_points] = waves - waves_hi
    wpad_ref[3 * qp:3 * qp + 1, :grid_points] = core_hi
    wpad_ref[3 * qp + 1:3 * qp + 2, :grid_points] = core_mid
    wpad_ref[3 * qp + 2:3 * qp + 3, :grid_points] = core - core_hi - core_mid
    wpad_ref[depth:depth + 1, :grid_points] = point_weight
    turned = wpad_ref[...].T
    forward = turned[:grid_points, :depth].astype(bf16)
    weight = turned[:grid_points, depth:depth + 1]
    wpad_ref[:qp, :] = jnp.zeros((qp, wpad_ref.shape[1]), f32)
    wpad_ref[:pairs, :grid_points] = waves * (-E2 * point_weight)
    b_hi, b_lo = two(wpad_ref[:qp, :grid_points])
    reverse = jnp.concatenate([b_hi.astype(f32), b_lo.astype(f32)], axis=0).astype(bf16)

    me = 2 * domain + band
    row = lax.broadcasted_iota(jnp.int32, (half, LANES), 0)
    held, begun = [], jnp.zeros((1, LANES), jnp.int32)
    for d in range(domains):
        value = all_ref[d][:1, :]
        held.append(jnp.maximum((value - ((me - begun) & (workers - 1)) + workers - 1) // workers, 0))
        begun = begun + value
    lane = lax.broadcasted_iota(jnp.int32, (half, atoms), 1)
    base = jnp.zeros((1, LANES), jnp.int32)
    for k in range(windows_all):
        rank = jnp.zeros((half, LANES), jnp.int32) + row % SUBLANES + base
        live = jnp.zeros((half, LANES), jnp.int32)
        for d in range(domains):
            here = jnp.clip(held[d] - SUBLANES * k, 0, SUBLANES)
            rank = rank + jnp.where(row >= (d + 1) * SUBLANES, here, 0)
            live = jnp.where(row // SUBLANES == d, here, live)
            base = base + here
        rank = jnp.where(row % SUBLANES < live, rank, -1)
        rank = jnp.concatenate([rank] * tiles, axis=1)
        sel_ref[k * half:(k + 1) * half, :] = jnp.where(rank == lane, 1.0, 0.0).astype(bf16)

    def deal(c):
        lanes = lanes_of(outward[c])
        sum_copy(c).wait_recv()
        send[c, :half, :lanes] += cross[c, :, :lanes]
        loop(1, lambda off: deal_copy(c, off).start())
        recv[c, mine, :lanes] = send[c, mine, :lanes]

    def take(c):
        deal_all(c).wait_recv()
        windows = outward[c]
        base = len(windows) * LANES
        tails = two(recv[c, :, base:base + LANES].T)
        for i, k in enumerate(windows):
            spot = slice(k * half, (k + 1) * half)
            mains = two(recv[c, :, i * LANES:(i + 1) * LANES].T)
            for e in range(2):
                stack_ref[e * packed:e * packed + LANES, spot] = mains[e]
                stack_ref[e * packed + LANES:(e + 1) * packed, spot] = tails[e][
                    i * TAIL:(i + 1) * TAIL
                ]

    def give(c, known):
        windows = homeward[c]
        base = len(windows) * LANES
        span = slice(0, known * LANES)
        tails = []
        for i, k in enumerate(windows):
            sel = sel_ref[k * half:(k + 1) * half, span]
            out = dot_last(sel, outs_ref[0, :, span]) + dot_last(sel, outs_ref[1, :, span])
            res_ref[c, :, i * LANES:(i + 1) * LANES] = out[:, :LANES]
            tails.append(out[:, LANES:])
        if len(windows) == 1:
            tails.append(jnp.zeros((half, TAIL), f32))
        res_ref[c, :, base:base + LANES] = jnp.concatenate(tails, axis=1)
        loop(1, lambda off: back_copy(c, off).start())
        got[c, mine, :base + LANES] = res_ref[c, mine, :base + LANES]

    def share(c):
        back_all(c).wait_recv()
        share_copy(c).start()

    def places(n):
        return [pl.ds(2 * n + i, qp, stride=np_) for i in range(2)]

    ones = jnp.ones((8, WIDE), f32)

    def enter(n, s):
        x = jnp.concatenate([flow_ref[at, :] for at in places(n)], axis=1)
        hi = x.astype(bf16).astype(f32)
        cols = jnp.concatenate([hi, x - hi, hi, ones], axis=0).astype(bf16)
        pts_ref[s] = jnp.dot(forward, cols, preferred_element_type=f32)

    def leave(n, s):
        both = jnp.dot(reverse, hi_ref[s], preferred_element_type=f32)
        out = both[:qp] + both[qp:] + jnp.dot(b_hi, lo_ref[s], preferred_element_type=f32)
        for i, at in enumerate(places(n)):
            back_ref[at, :] = out[:, i * LANES:(i + 1) * LANES]

    def evaluate(s):
        for g in range(0, grid_points, step):
            part = pl.ds(g, step)
            p = pts_ref[s, part, :]
            u = p * p + 0.25
            power = jnp.log2(u)
            t = jnp.exp2(power * (1.0 / 6.0))
            w = jnp.exp2(power * (-1.0 / 3.0))
            r = 1.0 / (t + C_RS / 7.8)
            eacc_ref[s % eacc_ref.shape[0], part, :] += (u * w) * (r + EX_A / E1)
            pot = (p * w) * ((r + E1 / E2) * r + EX_D / E2)
            hi = pot.astype(bf16)
            hi_ref[s, part, :] = hi
            lo_ref[s, part, :] = (pot - hi.astype(f32)).astype(bf16)

    def compute(i, services):
        rows = slice(0, -(-(i + 1) * windows_all // tiles) * half)
        span = slice(i * LANES, (i + 1) * LANES)
        sel = sel_ref[rows, span]
        picked = jnp.dot(stack_ref[:, rows], sel, preferred_element_type=f32).astype(bf16)
        hi, lo = picked[:packed], picked[packed:]
        coef_ref[...] = (
            jnp.dot(into_hi, hi, preferred_element_type=f32)
            + jnp.dot(into_hi, lo, preferred_element_type=f32)
            + jnp.dot(into_lo, hi, preferred_element_type=f32)
        )
        for group in groups:
            x = side_by_side(coef_ref, group, lp)
            flow = jnp.dot(y_in, terms(x), preferred_element_type=f32)
            for i, q in enumerate(group):
                flow_ref[q * np_:(q + 1) * np_, :] = flow[:np_, i * LANES:(i + 1) * LANES]
        eacc_ref[...] = jnp.zeros_like(eacc_ref)
        enter(0, 0)

        def body(turn, carry):
            for at, service in services:
                if at < couples // depth_of:
                    @pl.when(turn == at)
                    def _():
                        service()
            for s in range(depth_of):
                n = turn * depth_of + s
                enter(jnp.minimum(n + 1, couples - 1), (s + 1) % depth_of)
                leave(jnp.maximum(n - 1, 0), (s - 1) % depth_of)
                evaluate(s)
            return carry

        lax.fori_loop(0, couples // depth_of, body, 0)
        for at, service in services:
            if at >= couples // depth_of:
                service()
        leave(couples - 1, depth_of - 1)
        for group in groups:
            x = side_by_side(back_ref, group, np_)
            coef = jnp.dot(y_out, terms(x), preferred_element_type=f32)
            for i, q in enumerate(group):
                coef_ref[q * lp:(q + 1) * lp, :] = coef[:, i * LANES:(i + 1) * LANES]
        c_hi, c_lo = two(coef_ref[...])
        ham = jnp.dot(out_all, c_hi, preferred_element_type=f32)
        ham = ham[:packed] + ham[packed:] + jnp.dot(out_hi, c_lo, preferred_element_type=f32)
        total = eacc_ref[0]
        for s in range(1, eacc_ref.shape[0]):
            total = total + eacc_ref[s]
        total = jnp.sum(total * weight, axis=0, keepdims=True)
        energy = -E1 * (total[:, :LANES] + total[:, LANES:])
        ids = lax.broadcasted_iota(jnp.int32, (packed, LANES), 0)
        hi, lo = two(jnp.where(ids == entries, energy, ham))
        outs_ref[0, :, span] = hi
        outs_ref[1, :, span] = lo

    def last_needed(i):
        need = -(-(i + 1) * windows_all // tiles)
        return next(c for c, windows in enumerate(outward) if windows[-1] + 1 >= need)

    turns = couples // depth_of
    dealt_to, taken, given, shared = 0, 0, 0, 0
    for i in range(tiles):
        last = last_needed(i)
        while dealt_to <= last:
            deal(dealt_to)
            dealt_to += 1
        if i == 0 and dealt_to < len(outward):
            deal(dealt_to)
            dealt_to += 1
        while taken <= last:
            take(taken)
            taken += 1
        services = []
        if i == 0:
            for c in range(dealt_to, len(outward)):
                spot = 2 + 3 * (c - dealt_to)
                services.append((spot, lambda c=c: deal(c)))
            dealt_to = len(outward)
        for c in range(shared, given):
            services.append((min(turns - 1, 3), lambda c=c: share(c)))
        shared = given
        compute(i, services)
        while i + 1 < tiles and given < len(homeward):
            need = -(-half * (homeward[given][-1] + 1) // LANES)
            if min(need, tiles) > i + 1:
                break
            give(given, min(need, tiles))
            given += 1

    perm = perm_ref[...]

    def finish(c):
        share_copy(c).wait_recv()
        windows = homeward[c]
        base = len(windows) * LANES

        def spread(lanes):
            rows = jnp.concatenate([got[c, :, lanes], cross_back[c, :, lanes]], axis=0).T
            hi, lo = two(rows)
            return jnp.dot(hi, perm, preferred_element_type=f32) + jnp.dot(
                lo, perm, preferred_element_type=f32
            )

        tails = spread(slice(base, base + LANES))
        for i, k in enumerate(windows):
            part = pl.ds(k * width, width)
            ham_ref[:LANES, part] = spread(slice(i * LANES, (i + 1) * LANES))
            ham_ref[LANES:, part] = tails[i * TAIL:i * TAIL + extra]
            for j in range(width // LANES):
                line = k * (width // LANES) + j
                energy_ref[line:line + 1, :] = tails[
                    i * TAIL + extra:i * TAIL + extra + 1, j * LANES:(j + 1) * LANES
                ]

    def sent_out(c):
        deal_all(c).wait_send()
        sum_copy(c).wait_send()

    def sent_home(c):
        back_all(c).wait_send()

    finished, cleared = 0, 0
    for c in range(shared, len(homeward)):
        while given < min(c + AHEAD, len(homeward)):
            give(given, tiles)
            given += 1
        if c == shared:
            count_all().wait_send()
            for e in range(len(outward)):
                sent_out(e)
        share(c)
        if c:
            finish(finished)
            finished += 1
        if c > 1:
            sent_home(cleared)
            cleared += 1
    while cleared < len(homeward):
        sent_home(cleared)
        cleared += 1
    while finished < len(homeward):
        finish(finished)
        finished += 1
    for c in range(len(homeward)):
        share_copy(c).wait_send()

def local(memory):
    return pl.BlockSpec(memory_space=memory)

def dealt(dens_part, counts, gaunt, pair_waves, y_table, core, radial_weights):
    domains = lax.axis_size("domain")
    entries, slots = dens_part.shape[1:]
    pairs, grid_points = pair_waves.shape
    harmonics, directions = y_table.shape
    half = SUBLANES * domains
    width = 2 * half
    n = len(chunk_plan(slots, width, True))
    lanes = 3 * LANES
    atoms = slots // 3 // 2
    packed = LANES + TAIL
    vmem, smem = pltpu.VMEM, pltpu.SMEM
    dma = pltpu.SemaphoreType.DMA
    step = next(size for size in (STEP, 16, 8) if grid_points % size == 0)
    depth_of = next(size for size in (5, 4, 3, 2, 1) if directions // 2 % size == 0)
    qp, lp = round_up(pairs, 8), round_up(harmonics, 16)
    np_ = round_up(directions, 8)
    ham, energy = pl.pallas_call(
        lambda *refs: whole_kernel(*refs, step=step, domains=domains, depth_of=depth_of),
        out_shape=(
            jax.ShapeDtypeStruct((entries, slots), f32),
            jax.ShapeDtypeStruct((slots // LANES, LANES), f32),
        ),
        in_specs=[local(vmem), local(smem)] + [local(vmem)] * 5,
        out_specs=(local(vmem),) * 2,
        scratch_shapes=[
            vmem((SUBLANES, LANES), jnp.int32),
            vmem((domains, SUBLANES, LANES), jnp.int32),
            vmem((width, width), bf16),
            vmem((lanes, width), f32),
            vmem((n, width, lanes), f32),
            vmem((n, half, lanes), f32),
            vmem((n, half, lanes), f32),
            vmem((n, half, lanes), f32),
            vmem((n, half, lanes), f32),
            vmem((n, half, lanes), f32),
            vmem((slots // 2, atoms), bf16),
            vmem((2 * packed, slots // 2), bf16),
            vmem((packed, gaunt.shape[1]), f32),
            vmem((2 * LANES, LANES), f32),
            vmem((LANES, round_up(grid_points, LANES)), f32),
            vmem((pairs * lp, LANES), f32),
            vmem((qp * np_, LANES), f32),
            vmem((qp * np_, LANES), f32),
            vmem((depth_of, grid_points, WIDE), f32),
            vmem((depth_of, grid_points, WIDE), bf16),
            vmem((depth_of, grid_points, WIDE), bf16),
            vmem((2, grid_points, WIDE), f32),
            vmem((2, packed, atoms), bf16),
            dma(()), dma(()), dma((n,)), dma((n,)), dma((n,)), dma((n,)),
            dma((n,)), dma((n,)), dma((n,)), dma((n,)),
        ],
        compiler_params=pltpu.CompilerParams(
            collective_id=0, has_side_effects=True, vmem_limit_bytes=48 * 1024 * 1024
        ),
        name="whole",
    )(
        dens_part, counts, gaunt, pair_waves, y_table, core.reshape(1, grid_points),
        radial_weights.reshape(1, grid_points),
    )
    return ham, energy.reshape(slots)

def fits(bands, domains, entries, slots, pairs, grid_points, harmonics, directions):
    workers = bands * domains
    return (
        bands == 2
        and workers & (workers - 1) == 0
        and (SUBLANES * domains) % LANES == 0
        and slots % (SUBLANES * workers) == 0
        and slots % (3 * bands * LANES) == 0
        and LANES < entries < LANES + TAIL
        and directions % 2 == 0
        and max(3 * harmonics + 48, 2 * directions, 3 * pairs + 40) <= LANES
        and grid_points % SUBLANES == 0
    )

def solution(mesh):
    bands, domains = mesh.shape["band"], mesh.shape["domain"]

    def per_device(*arrays):
        entries, slots = arrays[0].shape[1:]
        sizes = arrays[3].shape + arrays[4].shape
        path = dealt if fits(bands, domains, entries, slots, *sizes) else general
        return path(*arrays)

    return jax.shard_map(
        per_device,
        mesh=mesh,
        in_specs=(P("band", None, "domain"), P("domain"), P(), P(), P(), P(), P()),
        out_specs=(P(None, "domain"), P("domain")),
        check_vma=False,
    )
```

```python
import math

import jax
import jax.numpy as jnp
from jax import lax
from jax.experimental import pallas as pl
from jax.experimental.pallas import tpu as pltpu
from jax.sharding import PartitionSpec as P

highest = lax.Precision.HIGHEST
f32 = jnp.float32
bf16 = jnp.bfloat16

LANES = 128
WIDE = 256

C_RS = 0.6203504908994
EX_A = 0.7385587663820224
EX_D = 0.9847450218426965

def round_up(value, step):
    return -(-value // step) * step

def split(x):
    hi = lax.reduce_precision(x, 8, 7)
    return hi.astype(bf16), (x - hi).astype(bf16)

def general_kernel(
    dens_ref, gy_ref, gyb_ref, pw_ref, pwb_ref, core_ref, weight_ref,
    ham_ref, energy_ref, pts_ref, hi_ref, lo_ref, eacc_ref, back_ref, *, pairs, step
):
    atoms = dens_ref.shape[1]
    rows = pw_ref.shape[1]
    grid_points = pw_ref.shape[0]
    couples = gy_ref.shape[0]
    chunks = 2 * atoms // WIDE
    eacc_ref[...] = jnp.zeros_like(eacc_ref)

    def mixed(x):
        ids = lax.broadcasted_iota(jnp.int32, x.shape, 0)
        hi = x.astype(bf16).astype(f32)
        low = (ids >= pairs) & (ids < 2 * pairs)
        return jnp.where(low, x - hi, hi).astype(bf16)

    def body(m, carry):
        both = jnp.dot(gy_ref[m], dens_ref[...], preferred_element_type=f32)
        lhs = mixed(jnp.concatenate([both[:rows], both[rows:]], axis=1))
        back = []
        for j in range(chunks):
            cols = lhs[:, j * WIDE:(j + 1) * WIDE]
            pts_ref[j] = jnp.dot(pw_ref[...], cols, preferred_element_type=f32)
            for g in range(0, grid_points, step):
                part = pl.ds(g, step)
                p = pts_ref[j, part, :] + core_ref[part, :]
                u = p * p + 0.25
                v = jnp.exp2(jnp.log(u) * (-1.0 / (6.0 * math.log(2.0))))
                r = v / (7.8 + C_RS * v)
                v2 = v * v
                br = 0.44 * r
                eacc_ref[j, part, :] += (u * v2) * (EX_A + br)
                pot = (p * v2) * (EX_D + (0.44 + (0.44 * C_RS / 3.0) * r) * r)
                hi = pot.astype(bf16)
                hi_ref[j, part, :] = hi
                lo_ref[j, part, :] = (pot - hi.astype(f32)).astype(bf16)
            first = jnp.dot(pwb_ref[...], hi_ref[j], preferred_element_type=f32)
            second = jnp.dot(pwb_ref[:rows, :], lo_ref[j], preferred_element_type=f32)
            back.append(first[:rows] + first[rows:] + second)
        back = mixed(jnp.concatenate(back, axis=1))
        start = pl.multiple_of(m * 2 * rows, 2 * rows)
        back_ref[pl.ds(start, rows), :] = back[:, :atoms]
        back_ref[pl.ds(start + rows, rows), :] = back[:, atoms:]
        return carry

    lax.fori_loop(0, couples, body, 0)
    ham_ref[...] = jnp.dot(gyb_ref[...], back_ref[...], preferred_element_type=f32)
    sums = [
        jnp.sum(eacc_ref[j] * weight_ref[...], axis=0, keepdims=True) for j in range(chunks)
    ]
    sums = jnp.concatenate(sums, axis=1)
    energy_ref[...] = jnp.broadcast_to(
        -(sums[:, :atoms] + sums[:, atoms:]), energy_ref.shape
    )

def general_tables(gaunt, pair_waves, y_table, core, radial_weights):
    entries = gaunt.shape[0]
    harmonics, directions = y_table.shape
    pairs, grid_points = pair_waves.shape
    rows = round_up(3 * pairs, 16)
    extra = rows - 3 * pairs
    assert directions % 2 == 0
    fused = jnp.einsum(
        "plq,ln->nqp", gaunt.reshape(entries, harmonics, pairs), y_table, precision=highest
    )

    hi, lo = split(fused)
    wide = lambda a, b, c: jnp.pad(
        jnp.concatenate([a, b, c], axis=1), ((0, 0), (0, extra), (0, 0))
    )
    hi3 = wide(hi, hi, hi)
    lo3 = wide(lo, lo, lo)
    gy = jnp.concatenate([hi3, hi3, lo3], axis=2).reshape(directions // 2, 2 * rows, 3 * entries)
    gyb = wide(hi, hi, lo).reshape(directions * rows, entries).T
    pw_hi, pw_lo = split(pair_waves)
    pw = jnp.pad(jnp.concatenate([pw_hi, pw_hi, pw_lo], axis=0), ((0, extra), (0, 0))).T
    point_weight = 4.0 * jnp.pi / directions * radial_weights
    b_hi, b_lo = split(-point_weight[None, :] * pair_waves)
    triple = lambda x: jnp.pad(jnp.concatenate([x, x, x], axis=0), ((0, extra), (0, 0)))
    pwb = jnp.concatenate([triple(b_hi), triple(b_lo)], axis=0)
    core_wide = jnp.broadcast_to(core[:, None], (grid_points, WIDE))
    weight_wide = jnp.broadcast_to(point_weight[:, None], (grid_points, WIDE))
    return gy, gyb, pw, pwb, core_wide, weight_wide

def general_energy(columns, tables, pairs):
    entries, atoms = columns.shape
    gy, gyb, pw, pwb, core_wide, weight_wide = tables
    grid_points, rows = pw.shape
    hi, lo = split(columns)
    dens = jnp.concatenate([hi, lo, hi], axis=0)
    chunks = 2 * atoms // WIDE
    step = 80 if grid_points % 80 == 0 else grid_points

    ham, energy = pl.pallas_call(
        lambda *refs: general_kernel(*refs, pairs=pairs, step=step),
        out_shape=(
            jax.ShapeDtypeStruct((entries, atoms), f32),
            jax.ShapeDtypeStruct((8, atoms), f32),
        ),
        scratch_shapes=[
            pltpu.VMEM((chunks, grid_points, WIDE), f32),
            pltpu.VMEM((chunks, grid_points, WIDE), bf16),
            pltpu.VMEM((chunks, grid_points, WIDE), bf16),
            pltpu.VMEM((chunks, grid_points, WIDE), f32),
            pltpu.VMEM((gyb.shape[1], atoms), bf16),
        ],
        compiler_params=pltpu.CompilerParams(vmem_limit_bytes=48 * 1024 * 1024),
        name="atoms",
    )(dens, gy, gyb, pw, pwb, core_wide, weight_wide)
    return ham, energy[:1]

def general(dens_part, counts, gaunt, pair_waves, y_table, core, radial_weights):
    band_count = lax.axis_size("band")
    domain_count = lax.axis_size("domain")
    workers = band_count * domain_count
    axes = ("domain", "band")
    me = lax.axis_index("domain") * band_count + lax.axis_index("band")
    entries = dens_part.shape[1]
    slot_total = dens_part.shape[2]
    share = slot_total // band_count
    capacity = -(-share // workers)
    worker_rows = -(-(slot_total // 3) // band_count)
    atoms = round_up(worker_rows, LANES)
    tables = general_tables(gaunt, pair_waves, y_table, core, radial_weights)

    own_cols = lax.psum_scatter(dens_part[0], "band", scatter_dimension=1, tiled=True)
    every_count = lax.all_gather(counts, "domain", axis=0, tiled=True)
    band_ids = jnp.arange(band_count, dtype=jnp.int32)
    live = jnp.clip(every_count[:, None] - band_ids[None, :] * share, 0, share).reshape(-1)
    ids = jnp.arange(workers, dtype=jnp.int32)
    starts = jnp.sum(jnp.where(ids[None, :] < ids[:, None], live[None, :], 0), axis=1)
    ends = starts + live
    own_start = jnp.sum(jnp.where(ids == me, starts, 0))
    own_live = jnp.sum(jnp.where(ids == me, live, 0))
    is_alive = jnp.arange(share, dtype=jnp.int32) < own_live

    own_cols = jnp.where(is_alive[None, :], own_cols, 0.0)
    own_cols = jnp.pad(own_cols, ((0, 0), (0, capacity * workers - share)))
    blocks = own_cols.T.reshape(capacity, workers, entries).transpose(1, 0, 2)
    outgoing = jnp.roll(blocks, own_start % workers, axis=0)
    incoming = lax.all_to_all(outgoing, axes, split_axis=0, concat_axis=0, tiled=True)

    atom_ids = jnp.arange(atoms, dtype=jnp.int32) * workers + me
    source = jnp.sum((ends[None, :] <= atom_ids[:, None]).astype(jnp.int32), axis=1)
    source = jnp.minimum(source, workers - 1)
    source_start = jnp.sum(jnp.where(source[:, None] == ids[None, :], starts[None, :], 0), axis=1)
    position = jnp.clip((atom_ids - source_start) // workers, 0, capacity - 1)
    compact = jnp.take(
        incoming.reshape(workers * capacity, entries), source * capacity + position, axis=0,
        mode="clip",
    )
    ham, energy = general_energy(compact.T, tables, pair_waves.shape[0])
    result = jnp.concatenate([ham, energy], axis=0).T
    row = (me - starts) % workers
    first = (starts + row - me) // workers
    target = first[:, None] + jnp.arange(capacity, dtype=jnp.int32)[None, :]
    back = jnp.take(result, jnp.clip(target, 0, atoms - 1).reshape(-1), axis=0, mode="clip")
    returned = lax.all_to_all(
        back.reshape(workers, capacity, entries + 1), axes, split_axis=0, concat_axis=0, tiled=True
    )
    returned = jnp.roll(returned, -(own_start % workers), axis=0)
    piece = returned.transpose(1, 0, 2).reshape(capacity * workers, entries + 1)[:share]
    piece = jnp.where(is_alive[:, None], piece, 0.0)
    band = lax.axis_index("band")
    whole = jnp.zeros((slot_total, entries + 1), f32)
    ring = [(i, (i + 1) % band_count) for i in range(band_count)]
    for hop in range(band_count):
        owner = (band - hop) % band_count
        whole = lax.dynamic_update_slice(whole, piece, (owner * share, 0))
        if hop + 1 < band_count:
            piece = lax.ppermute(piece, "band", ring)
    whole = whole.T
    return whole[:entries], whole[entries]

MESH = pl.DeviceIdType.MESH
SUBLANES = 8
TAIL = 64
STEP = 80
EAGER = True
SPOT = 2
AHEAD = 2
E1 = 0.44 / 7.8
E2 = 0.44 * C_RS / (3.0 * 7.8 * 7.8)

def chunk_plan(slots, width, odd_first):
    windows = slots // width
    lead = windows % 2 if odd_first else 0
    pieces = [range(lead)] if lead else []
    return pieces + [range(k, min(k + 2, windows)) for k in range(lead, windows, 2)]

def dot_last(a, b):
    return lax.dot_general(a, b, (((1,), (1,)), ((), ())), preferred_element_type=f32)

def two(x):
    hi = x.astype(bf16)
    return hi, (x - hi.astype(f32)).astype(bf16)

def greet(domains, domain, band):
    barrier = pltpu.get_barrier_semaphore()

    def hello(off, carry):
        peer = lax.rem(domain + off, domains)
        pl.semaphore_signal(barrier, inc=1, device_id=(band, peer), device_id_type=MESH)
        return carry

    lax.fori_loop(1, domains, hello, 0)
    pl.semaphore_signal(barrier, inc=1, device_id=(1 - band, domain), device_id_type=MESH)
    pl.semaphore_wait(barrier, domains)

def whole_kernel(
    dens_ref, cnt_ref, gaunt_ref, waves_ref, y_ref, core_ref, radial_ref,
    ham_ref, energy_ref,
    own_ref, all_ref, perm_ref, stage, send, cross, recv, res_ref, got, cross_back,
    sel_ref, stack_ref, gpad_ref, ypad_ref, wpad_ref, coef_ref, end_ref, flow_ref, back_ref,
    pts_ref, hi_ref, lo_ref, eacc_ref, outs_ref,
    cnt_out, cnt_in, x_out, x_in, a_out, a_in, rx_out, rx_in, ra_out, ra_in,
    *, step, domains, depth_of
):
    band, domain = lax.axis_index("band"), lax.axis_index("domain")
    entries, slots = dens_ref.shape[1:]
    fields = gaunt_ref.shape[1]
    pairs, grid_points = waves_ref.shape
    harmonics, directions = y_ref.shape
    workers = 2 * domains
    half = SUBLANES * domains
    width = 2 * half
    windows_all = slots // width
    outward = chunk_plan(slots, width, True)
    homeward = chunk_plan(slots, width, False)
    extra = entries - LANES
    atoms = sel_ref.shape[1]
    tiles = atoms // LANES
    qp, lp, np_ = round_up(pairs, 8), round_up(harmonics, 16), round_up(directions, 8)
    nn = round_up(directions, 16)
    depth = 3 * qp + 8
    packed = LANES + TAIL
    couples = directions // 2
    mine = pl.ds(pl.multiple_of(domain * SUBLANES, SUBLANES), SUBLANES)

    def loop(first, function):
        for off in range(first, domains):
            function(off)

    def lanes_of(windows):
        return (len(windows) + 1) * LANES

    def count_copy(off):
        peer = lax.rem(domain + off, domains)
        return pltpu.make_async_remote_copy(
            src_ref=own_ref, dst_ref=all_ref.at[domain], send_sem=cnt_out,
            recv_sem=cnt_in, device_id=(band, peer), device_id_type=MESH,
        )

    def pair_copy(source, target, c, windows, out_sem, in_sem, first):
        lanes = pl.ds(0, lanes_of(windows))
        return pltpu.make_async_remote_copy(
            src_ref=source.at[c, pl.ds(first, half), lanes],
            dst_ref=target.at[c, :, lanes], send_sem=out_sem.at[c],
            recv_sem=in_sem.at[c], device_id=(1 - band, domain), device_id_type=MESH,
        )

    def plane_copy(source, target, c, windows, out_sem, in_sem, off):
        lanes = pl.ds(0, lanes_of(windows))
        peer = lax.rem(domain + off, domains)
        rows = pl.ds(pl.multiple_of(peer * SUBLANES, SUBLANES), SUBLANES)
        return pltpu.make_async_remote_copy(
            src_ref=source.at[c, rows, lanes],
            dst_ref=target.at[c, mine, lanes], send_sem=out_sem.at[c],
            recv_sem=in_sem.at[c], device_id=(band, peer), device_id_type=MESH,
        )

    def count_all():
        others = pl.ds(0, domains - 1)
        return pltpu.make_async_remote_copy(
            src_ref=all_ref.at[others], dst_ref=all_ref.at[others], send_sem=cnt_out,
            recv_sem=cnt_in, device_id=(1 - band, domain), device_id_type=MESH,
        )

    def plane_all(source, target, c, windows, out_sem, in_sem):
        lanes = pl.ds(0, lanes_of(windows))
        rows = pl.ds(0, half - SUBLANES)
        return pltpu.make_async_remote_copy(
            src_ref=source.at[c, rows, lanes], dst_ref=target.at[c, rows, lanes],
            send_sem=out_sem.at[c], recv_sem=in_sem.at[c],
            device_id=(1 - band, domain), device_id_type=MESH,
        )

    def deal_all(c):
        return plane_all(send, recv, c, outward[c], a_out, a_in)

    def back_all(c):
        return plane_all(res_ref, got, c, homeward[c], ra_out, ra_in)

    def sum_copy(c):
        return pair_copy(send, cross, c, outward[c], x_out, x_in, half)

    def deal_copy(c, off):
        return plane_copy(send, recv, c, outward[c], a_out, a_in, off)

    def back_copy(c, off):
        return plane_copy(res_ref, got, c, homeward[c], ra_out, ra_in, off)

    def share_copy(c):
        return pair_copy(got, cross_back, c, homeward[c], rx_out, rx_in, 0)

    greet(domains, domain, band)
    own_ref[...] = jnp.full((1, LANES), cnt_ref[0], jnp.int32)
    loop(1, lambda off: count_copy(off).start())
    all_ref[domain] = own_ref[...]
    stage[...] = jnp.zeros_like(stage)
    hi_ref[...] = jnp.zeros_like(hi_ref)
    lo_ref[...] = jnp.zeros_like(lo_ref)
    back_ref[...] = jnp.zeros_like(back_ref)
    flow_ref[...] = jnp.zeros_like(flow_ref)
    gpad_ref[...] = jnp.zeros_like(gpad_ref)
    ypad_ref[...] = jnp.zeros_like(ypad_ref)
    wpad_ref[...] = jnp.zeros_like(wpad_ref)
    count_all().wait_recv()
    start = jnp.zeros((1, LANES), jnp.int32)
    for d in range(domains):
        start = start + jnp.where(d < domain, all_ref[d], 0)
    start = start[:1, :1]
    row = lax.broadcasted_iota(jnp.int32, (width, width), 0)
    slot = lax.broadcasted_iota(jnp.int32, (width, width), 1)
    own = row < half
    row = jnp.where(own, row, row - half)
    worker = 2 * (row // SUBLANES) + jnp.where(own, band, 1 - band)
    source = ((worker - start) & (workers - 1)) + workers * (row % SUBLANES)
    perm = jnp.where(slot == source, 1.0, 0.0).astype(bf16)
    perm_ref[...] = perm
    for c, windows in enumerate(outward):
        base = len(windows) * LANES
        for i, k in enumerate(windows):
            part = pl.ds(k * width, width)
            stage[i * LANES:(i + 1) * LANES, :] = dens_ref[0, :LANES, part]
            stage[base + i * TAIL:base + i * TAIL + extra, :] = dens_ref[0, LANES:, part]
            rest = slice(base + i * TAIL + extra, base + (i + 1) * TAIL)
            stage[rest, :] = jnp.zeros((TAIL - extra, width), f32)
        if len(windows) == 1:
            stage[base + TAIL:base + 2 * TAIL, :] = jnp.zeros((TAIL, width), f32)
        hi, lo = two(stage[:base + LANES, :])
        send[c, :, :base + LANES] = dot_last(perm, hi) + dot_last(perm, lo)
        sum_copy(c).start()

    groups = [range(q, min(q + 2, pairs)) for q in range(0, pairs, 2)]

    def side_by_side(ref, group, size):
        return jnp.concatenate([ref[q * size:(q + 1) * size, :] for q in group], axis=1)

    def terms(x):
        hi = x.astype(bf16).astype(f32)
        return jnp.concatenate([hi, x - hi, hi], axis=0).astype(bf16)

    gpad_ref[:entries, :] = gaunt_ref[...]
    r = lax.broadcasted_iota(jnp.int32, (pairs * lp, fields), 0)
    col = lax.broadcasted_iota(jnp.int32, (pairs * lp, fields), 1)
    wanted = jnp.where(r % lp < harmonics, (r % lp) * pairs + r // lp, -1)
    order = jnp.where(wanted == col, 1.0, 0.0).astype(bf16)
    g_hi, g_lo = two(gpad_ref[...])
    into_hi, into_lo = dot_last(order, g_hi).astype(bf16), dot_last(order, g_lo).astype(bf16)
    out_hi, out_lo = dot_last(g_hi, order).astype(bf16), dot_last(g_lo, order).astype(bf16)
    out_all = jnp.concatenate([out_hi, out_lo], axis=0)
    y = y_ref[...]
    near = y.astype(bf16).astype(f32)
    for i, part in enumerate((near, near, y - near)):
        ypad_ref[i * lp:i * lp + harmonics, :directions] = part
    turned = ypad_ref[...].T
    y_in = turned[:nn, :3 * lp].astype(bf16)
    blocks = [turned[:np_, i * lp:(i + 1) * lp] for i in range(3)]
    ypad_ref[...] = jnp.zeros_like(ypad_ref)
    for i, part in enumerate(blocks):
        ypad_ref[i * np_:(i + 1) * np_, :lp] = part
    y_out = ypad_ref[...].T[:lp, :3 * np_].astype(bf16)

    point_weight = (4.0 * math.pi / directions) * radial_ref[...]
    waves = waves_ref[...]
    waves_hi = waves.astype(bf16).astype(f32)
    core = core_ref[...]
    core_hi = core.astype(bf16).astype(f32)
    core_mid = (core - core_hi).astype(bf16).astype(f32)
    wpad_ref[:pairs, :grid_points] = waves_hi
    wpad_ref[qp:qp + pairs, :grid_points] = waves_hi
    wpad_ref[2 * qp:2 * qp + pairs, :grid_points] = waves - waves_hi
    wpad_ref[3 * qp:3 * qp + 1, :grid_points] = core_hi
    wpad_ref[3 * qp + 1:3 * qp + 2, :grid_points] = core_mid
    wpad_ref[3 * qp + 2:3 * qp + 3, :grid_points] = core - core_hi - core_mid
    wpad_ref[depth:depth + 1, :grid_points] = point_weight
    turned = wpad_ref[...].T
    forward = turned[:grid_points, :depth].astype(bf16)
    weight = turned[:grid_points, depth:depth + 1]
    wpad_ref[:qp, :] = jnp.zeros((qp, wpad_ref.shape[1]), f32)
    wpad_ref[:pairs, :grid_points] = waves * (-E2 * point_weight)
    b_hi, b_lo = two(wpad_ref[:qp, :grid_points])
    reverse = jnp.concatenate([b_hi.astype(f32), b_lo.astype(f32)], axis=0).astype(bf16)

    me = 2 * domain + band
    row = lax.broadcasted_iota(jnp.int32, (half, LANES), 0)
    held, begun = [], jnp.zeros((1, LANES), jnp.int32)
    for d in range(domains):
        value = all_ref[d][:1, :]
        held.append(jnp.maximum((value - ((me - begun) & (workers - 1)) + workers - 1) // workers, 0))
        begun = begun + value
    lane = lax.broadcasted_iota(jnp.int32, (half, atoms), 1)
    base = jnp.zeros((1, LANES), jnp.int32)
    for k in range(windows_all):
        rank = jnp.zeros((half, LANES), jnp.int32) + row % SUBLANES + base
        live = jnp.zeros((half, LANES), jnp.int32)
        for d in range(domains):
            here = jnp.clip(held[d] - SUBLANES * k, 0, SUBLANES)
            rank = rank + jnp.where(row >= (d + 1) * SUBLANES, here, 0)
            live = jnp.where(row // SUBLANES == d, here, live)
            base = base + here
        rank = jnp.where(row % SUBLANES < live, rank, -1)
        rank = jnp.concatenate([rank] * tiles, axis=1)
        sel_ref[k * half:(k + 1) * half, :] = jnp.where(rank == lane, 1.0, 0.0).astype(bf16)

    def deal(c):
        lanes = lanes_of(outward[c])
        sum_copy(c).wait_recv()
        send[c, :half, :lanes] += cross[c, :, :lanes]
        loop(1, lambda off: deal_copy(c, off).start())
        recv[c, mine, :lanes] = send[c, mine, :lanes]

    def take(c):
        deal_all(c).wait_recv()
        windows = outward[c]
        base = len(windows) * LANES
        tails = two(recv[c, :, base:base + LANES].T)
        for i, k in enumerate(windows):
            spot = slice(k * half, (k + 1) * half)
            mains = two(recv[c, :, i * LANES:(i + 1) * LANES].T)
            for e in range(2):
                stack_ref[e * packed:e * packed + LANES, spot] = mains[e]
                stack_ref[e * packed + LANES:(e + 1) * packed, spot] = tails[e][
                    i * TAIL:(i + 1) * TAIL
                ]

    def give(c, known):
        windows = homeward[c]
        base = len(windows) * LANES
        span = slice(0, known * LANES)
        tails = []
        for i, k in enumerate(windows):
            sel = sel_ref[k * half:(k + 1) * half, span]
            out = dot_last(sel, outs_ref[0, :, span]) + dot_last(sel, outs_ref[1, :, span])
            res_ref[c, :, i * LANES:(i + 1) * LANES] = out[:, :LANES]
            tails.append(out[:, LANES:])
        if len(windows) == 1:
            tails.append(jnp.zeros((half, TAIL), f32))
        res_ref[c, :, base:base + LANES] = jnp.concatenate(tails, axis=1)
        loop(1, lambda off: back_copy(c, off).start())
        got[c, mine, :base + LANES] = res_ref[c, mine, :base + LANES]

    def share(c):
        back_all(c).wait_recv()
        share_copy(c).start()

    def places(n):
        return [pl.ds(2 * n + i, qp, stride=np_) for i in range(2)]

    ones = jnp.ones((8, WIDE), f32)

    def enter(n, s):
        x = jnp.concatenate([flow_ref[at, :] for at in places(n)], axis=1)
        hi = x.astype(bf16).astype(f32)
        cols = jnp.concatenate([hi, x - hi, hi, ones], axis=0).astype(bf16)
        pts_ref[s, :grid_points, :] = jnp.dot(forward, cols, preferred_element_type=f32)

    def leave(n, s):
        both = jnp.dot(reverse, hi_ref[s, :grid_points, :], preferred_element_type=f32)
        out = both[:qp] + both[qp:] + jnp.dot(b_hi, lo_ref[s, :grid_points, :], preferred_element_type=f32)
        for i, at in enumerate(places(n)):
            back_ref[at, :] = out[:, i * LANES:(i + 1) * LANES]

    def evaluate(s):
        for g in range(0, grid_points, step):
            part = pl.ds(g, step)
            p = pts_ref[s, part, :]
            u = p * p + 0.25
            power = jnp.log2(u)
            t = jnp.exp2(power * (1.0 / 6.0))
            w = jnp.exp2(power * (-1.0 / 3.0))
            r = 1.0 / (t + C_RS / 7.8)
            eacc_ref[s % eacc_ref.shape[0], part, :] += (u * w) * (r + EX_A / E1)
            pot = (p * w) * ((r + E1 / E2) * r + EX_D / E2)
            hi = pot.astype(bf16)
            hi_ref[s, part, :] = hi
            lo_ref[s, part, :] = (pot - hi.astype(f32)).astype(bf16)

    def prologue(i):
        rows = slice(0, -(-(i + 1) * windows_all // tiles) * half)
        span = slice(i * LANES, (i + 1) * LANES)
        sel = sel_ref[rows, span]
        picked = jnp.dot(stack_ref[:, rows], sel, preferred_element_type=f32).astype(bf16)
        hi, lo = picked[:packed], picked[packed:]
        coef_ref[...] = (
            jnp.dot(into_hi, hi, preferred_element_type=f32)
            + jnp.dot(into_hi, lo, preferred_element_type=f32)
            + jnp.dot(into_lo, hi, preferred_element_type=f32)
        )
        for group in groups:
            x = side_by_side(coef_ref, group, lp)
            flow = jnp.dot(y_in, terms(x), preferred_element_type=f32)
            for e, q in enumerate(group):
                flow_ref[q * np_:(q + 1) * np_, :] = flow[:np_, e * LANES:(e + 1) * LANES]
        eacc_ref[...] = jnp.zeros_like(eacc_ref)
        enter(0, 0)

    def main(services):
        def body(turn, carry):
            for at, service in services:
                if at < couples // depth_of:
                    @pl.when(turn == at)
                    def _():
                        service()
            for s in range(depth_of):
                n = turn * depth_of + s
                enter(jnp.minimum(n + 1, couples - 1), (s + 1) % depth_of)
                leave(jnp.maximum(n - 1, 0), (s - 1) % depth_of)
                evaluate(s)
            return carry

        lax.fori_loop(0, couples // depth_of, body, 0)
        for at, service in services:
            if at >= couples // depth_of:
                service()
        leave(couples - 1, depth_of - 1)

    def epilogue(i):
        span = slice(i * LANES, (i + 1) * LANES)
        for group in groups:
            x = side_by_side(back_ref, group, np_)
            coef = jnp.dot(y_out, terms(x), preferred_element_type=f32)
            for e, q in enumerate(group):
                end_ref[q * lp:(q + 1) * lp, :] = coef[:, e * LANES:(e + 1) * LANES]
        c_hi, c_lo = two(end_ref[...])
        ham = jnp.dot(out_all, c_hi, preferred_element_type=f32)
        ham = ham[:packed] + ham[packed:] + jnp.dot(out_hi, c_lo, preferred_element_type=f32)
        total = eacc_ref[0, :grid_points, :]
        for s in range(1, eacc_ref.shape[0]):
            total = total + eacc_ref[s, :grid_points, :]
        total = jnp.sum(total * weight, axis=0, keepdims=True)
        energy = -E1 * (total[:, :LANES] + total[:, LANES:])
        ids = lax.broadcasted_iota(jnp.int32, (packed, LANES), 0)
        hi, lo = two(jnp.where(ids == entries, energy, ham))
        outs_ref[0, :, span] = hi
        outs_ref[1, :, span] = lo

    def last_needed(i):
        need = -(-(i + 1) * windows_all // tiles)
        return next(c for c, windows in enumerate(outward) if windows[-1] + 1 >= need)

    turns = couples // depth_of
    dealt_to, taken, given, shared = 0, 0, 0, 0
    for i in range(tiles):
        last = last_needed(i)
        while dealt_to <= last:
            deal(dealt_to)
            dealt_to += 1
        if i == 0 and dealt_to < len(outward) and EAGER:
            deal(dealt_to)
            dealt_to += 1
        while taken <= last:
            take(taken)
            taken += 1
        if i:
            epilogue(i - 1)
        prologue(i)
        while i and given < len(homeward):
            need = -(-half * (homeward[given][-1] + 1) // LANES)
            if min(need, tiles) > i:
                break
            give(given, min(need, tiles))
            given += 1
        services = []
        if i == 0:
            for c in range(dealt_to, len(outward)):
                services.append((SPOT + 3 * (c - dealt_to), lambda c=c: deal(c)))
            dealt_to = len(outward)
        for c in range(shared, given):
            services.append((min(turns - 1, 3), lambda c=c: share(c)))
        shared = given
        main(services)
    epilogue(tiles - 1)

    perm = perm_ref[...]

    def finish(c):
        share_copy(c).wait_recv()
        windows = homeward[c]
        base = len(windows) * LANES

        def spread(lanes):
            rows = jnp.concatenate([got[c, :, lanes], cross_back[c, :, lanes]], axis=0).T
            hi, lo = two(rows)
            return jnp.dot(hi, perm, preferred_element_type=f32) + jnp.dot(
                lo, perm, preferred_element_type=f32
            )

        tails = spread(slice(base, base + LANES))
        for i, k in enumerate(windows):
            part = pl.ds(k * width, width)
            ham_ref[:LANES, part] = spread(slice(i * LANES, (i + 1) * LANES))
            ham_ref[LANES:, part] = tails[i * TAIL:i * TAIL + extra]
            for j in range(width // LANES):
                line = k * (width // LANES) + j
                energy_ref[line:line + 1, :] = tails[
                    i * TAIL + extra:i * TAIL + extra + 1, j * LANES:(j + 1) * LANES
                ]

    def sent_out(c):
        deal_all(c).wait_send()
        sum_copy(c).wait_send()

    def sent_home(c):
        back_all(c).wait_send()

    finished, cleared = 0, 0
    for c in range(shared, len(homeward)):
        while given < min(c + AHEAD, len(homeward)):
            give(given, tiles)
            given += 1
        if c == shared:
            count_all().wait_send()
            for e in range(len(outward)):
                sent_out(e)
        share(c)
        if c:
            finish(finished)
            finished += 1
        if c > 1:
            sent_home(cleared)
            cleared += 1
    while cleared < len(homeward):
        sent_home(cleared)
        cleared += 1
    while finished < len(homeward):
        finish(finished)
        finished += 1
    for c in range(len(homeward)):
        share_copy(c).wait_send()

def local(memory):
    return pl.BlockSpec(memory_space=memory)

def dealt(dens_part, counts, gaunt, pair_waves, y_table, core, radial_weights):
    domains = lax.axis_size("domain")
    entries, slots = dens_part.shape[1:]
    pairs, grid_points = pair_waves.shape
    harmonics, directions = y_table.shape
    half = SUBLANES * domains
    width = 2 * half
    n = len(chunk_plan(slots, width, True))
    lanes = 3 * LANES
    atoms = slots // 3 // 2
    packed = LANES + TAIL
    vmem, smem = pltpu.VMEM, pltpu.SMEM
    dma = pltpu.SemaphoreType.DMA
    step = next(size for size in (STEP, 16, 8) if grid_points % size == 0)
    depth_of = next(size for size in (5, 4, 3, 2, 1) if directions // 2 % size == 0)
    qp, lp = round_up(pairs, 8), round_up(harmonics, 16)
    np_ = round_up(directions, 8)
    ham, energy = pl.pallas_call(
        lambda *refs: whole_kernel(*refs, step=step, domains=domains, depth_of=depth_of),
        out_shape=(
            jax.ShapeDtypeStruct((entries, slots), f32),
            jax.ShapeDtypeStruct((slots // LANES, LANES), f32),
        ),
        in_specs=[local(vmem), local(smem)] + [local(vmem)] * 5,
        out_specs=(local(vmem),) * 2,
        scratch_shapes=[
            vmem((1, LANES), jnp.int32),
            vmem((domains, 1, LANES), jnp.int32),
            vmem((width, width), bf16),
            vmem((lanes, width), f32),
            vmem((n, width, lanes), f32),
            vmem((n, half, lanes), f32),
            vmem((n, half, lanes), f32),
            vmem((n, half, lanes), f32),
            vmem((n, half, lanes), f32),
            vmem((n, half, lanes), f32),
            vmem((slots // 2, atoms), bf16),
            vmem((2 * packed, slots // 2), bf16),
            vmem((packed, gaunt.shape[1]), f32),
            vmem((2 * LANES, LANES), f32),
            vmem((LANES, round_up(grid_points, LANES)), f32),
            vmem((pairs * lp, LANES), f32),
            vmem((pairs * lp, LANES), f32),
            vmem((qp * np_, LANES), f32),
            vmem((qp * np_, LANES), f32),
            vmem((depth_of, grid_points + 8, WIDE), f32),
            vmem((depth_of, grid_points + 16, WIDE), bf16),
            vmem((depth_of, grid_points + 16, WIDE), bf16),
            vmem((2, grid_points + 8, WIDE), f32),
            vmem((2, packed, atoms), bf16),
            dma(()), dma(()), dma((n,)), dma((n,)), dma((n,)), dma((n,)),
            dma((n,)), dma((n,)), dma((n,)), dma((n,)),
        ],
        compiler_params=pltpu.CompilerParams(
            collective_id=0, has_side_effects=True, vmem_limit_bytes=48 * 1024 * 1024
        ),
        name="whole",
    )(
        dens_part, counts, gaunt, pair_waves, y_table, core.reshape(1, grid_points),
        radial_weights.reshape(1, grid_points),
    )
    return ham, energy.reshape(slots)

def fits(bands, domains, entries, slots, pairs, grid_points, harmonics, directions):
    workers = bands * domains
    return (
        bands == 2
        and workers & (workers - 1) == 0
        and (SUBLANES * domains) % LANES == 0
        and slots % (SUBLANES * workers) == 0
        and slots % (3 * bands * LANES) == 0
        and LANES < entries < LANES + TAIL
        and directions % 2 == 0
        and max(3 * harmonics + 48, 2 * directions, 3 * pairs + 40) <= LANES
        and grid_points % SUBLANES == 0
    )

def solution(mesh):
    bands, domains = mesh.shape["band"], mesh.shape["domain"]

    def per_device(*arrays):
        entries, slots = arrays[0].shape[1:]
        sizes = arrays[3].shape + arrays[4].shape
        path = dealt if fits(bands, domains, entries, slots, *sizes) else general
        return path(*arrays)

    return jax.shard_map(
        per_device,
        mesh=mesh,
        in_specs=(P("band", None, "domain"), P("domain"), P(), P(), P(), P(), P()),
        out_specs=(P(None, "domain"), P("domain")),
        check_vma=False,
    )
```
